16 devices in a mesh: pp: 2 (over z), dp: 8 (over y, x, core).
Axes of the slice: x: 2, y: 2, z: 2, core: 2. Of those that a mesh axis runs over, the one named last changes fastest.
Arguments:
- w_in: bfloat16 [2, 16, 256, 1024], P('pp')
- w_out: bfloat16 [2, 16, 1024, 256], P('pp')
- x_saved: bfloat16 [2, 2, 16, 4096, 256], P('pp', None, None, 'dp')
- h_saved: bfloat16 [2, 2, 16, 4096, 1024], P('pp', None, None, 'dp')
- dy_in: bfloat16 [2, 4096, 256], P('pp', 'dp')
- acc_in: float32 [2, 8, 16, 256, 1024], P('pp', 'dp')
- acc_out: float32 [2, 8, 16, 1024, 256], P('pp', 'dp')
Outputs:
- output 1: float32 [2, 16, 256, 1024], P('pp')
- output 2: float32 [2, 16, 1024, 256], P('pp')
- output 3: bfloat16 [2, 4096, 256], P('pp', 'dp')
All inputs are finite; a program needn't handle non-finite values.
Results may differ from the reference program's by a relative error of at most 0.0117373.
Values are sent between devices in bfloat16 or wider.
A program may use at most 1 GiB of HBM per device.

```python
import jax
import jax.numpy as jnp
from jax import lax

STAGES = 2
REPLICAS = 8
LAYERS_STAGE = 16
TOKENS_DEV = 512
HIDDEN = 256
FF_WIDTH = 1024

ROWS = REPLICAS * TOKENS_DEV
TOTAL_DEPTH = STAGES * LAYERS_STAGE


def setup_inputs(seed: int = 0) -> dict:
    key_list = jax.random.split(jax.random.key(seed), 7)
    tok_factor = TOKENS_DEV ** 0.5
    pending = (STAGES - jnp.arange(STAGES)).astype(jnp.float32)
    scale_in = jnp.sqrt(pending * tok_factor / (8.0 * TOTAL_DEPTH)).reshape(STAGES, 1, 1, 1, 1)
    scale_out = (0.65 * jnp.sqrt(pending * tok_factor)).reshape(STAGES, 1, 1, 1, 1)
    w_in = jax.random.normal(key_list[0], (STAGES, LAYERS_STAGE, HIDDEN, FF_WIDTH), jnp.float32) * HIDDEN ** -0.5
    w_out = jax.random.normal(key_list[1], (STAGES, LAYERS_STAGE, FF_WIDTH, HIDDEN), jnp.float32) * (FF_WIDTH * TOTAL_DEPTH) ** -0.5
    x_saved = jax.random.normal(key_list[2], (STAGES, STAGES, LAYERS_STAGE, ROWS, HIDDEN), jnp.float32)
    h_saved = jax.random.normal(key_list[3], (STAGES, STAGES, LAYERS_STAGE, ROWS, FF_WIDTH), jnp.float32)
    dy_in = jax.random.normal(key_list[4], (STAGES, ROWS, HIDDEN), jnp.float32) * TOKENS_DEV ** -0.25
    acc_in = jax.random.normal(key_list[5], (STAGES, REPLICAS, LAYERS_STAGE, HIDDEN, FF_WIDTH), jnp.float32) * scale_in
    acc_out = jax.random.normal(key_list[6], (STAGES, REPLICAS, LAYERS_STAGE, FF_WIDTH, HIDDEN), jnp.float32) * scale_out
    return {'w_in': w_in.astype(jnp.bfloat16), 'w_out': w_out.astype(jnp.bfloat16), 'x_saved': x_saved.astype(jnp.bfloat16), 'h_saved': h_saved.astype(jnp.bfloat16), 'dy_in': dy_in.astype(jnp.bfloat16), 'acc_in': acc_in, 'acc_out': acc_out}


def layer_backward(w_first, w_second, x_in, h_pre, cot_in):
    act_val, act_vjp = jax.vjp(jax.nn.gelu, h_pre.astype(jnp.float32))
    act_bf = act_val.astype(jnp.bfloat16)
    d_act = jnp.dot(cot_in, w_second.T, preferred_element_type=jnp.float32)
    d_pre = act_vjp(d_act)[0].astype(jnp.bfloat16)
    x_rows = x_in.reshape(REPLICAS, TOKENS_DEV, HIDDEN).astype(jnp.float32)
    pre_rows = d_pre.reshape(REPLICAS, TOKENS_DEV, FF_WIDTH).astype(jnp.float32)
    act_rows = act_bf.reshape(REPLICAS, TOKENS_DEV, FF_WIDTH).astype(jnp.float32)
    cot_rows = cot_in.reshape(REPLICAS, TOKENS_DEV, HIDDEN).astype(jnp.float32)
    grad_first = jnp.einsum('rtd,rtf->rdf', x_rows, pre_rows)
    grad_second = jnp.einsum('rtf,rtd->rfd', act_rows, cot_rows)
    back_sum = jnp.dot(d_pre, w_first.T, preferred_element_type=jnp.float32)
    cot_out = (cot_in.astype(jnp.float32) + back_sum).astype(jnp.bfloat16)
    return cot_out, grad_first, grad_second


def stage_backward(w_first, w_second, x_stage, h_stage, cot_in):
    def layer_body(cot_carry, layer_data):
        cot_next, grad_first, grad_second = layer_backward(layer_data[0], layer_data[1], layer_data[2], layer_data[3], cot_carry)
        return cot_next, (grad_first, grad_second)
    cot_out, grad_stack = lax.scan(layer_body, cot_in, (w_first, w_second, x_stage, h_stage), reverse=True)
    return cot_out, grad_stack[0], grad_stack[1]


def reference(w_in, w_out, x_saved, h_saved, dy_in, acc_in, acc_out):
    def stage_body(step_id, loop_state):
        cot_stack, grad_in, grad_out = loop_state
        stage_id = STAGES - 1 - step_id
        cot_stack = lax.dynamic_update_index_in_dim(cot_stack, dy_in[stage_id], stage_id, 0)
        w_first = w_in[stage_id]
        w_second = w_out[stage_id]
        x_stage = x_saved[stage_id]
        h_stage = h_saved[stage_id]

        def micro_body(slot_id, inner_state):
            cot_list, acc_first, acc_second = inner_state
            micro_id = stage_id + slot_id
            cot_out, grad_first, grad_second = stage_backward(w_first, w_second, x_stage[slot_id], h_stage[slot_id], cot_list[micro_id])
            cot_list = lax.dynamic_update_index_in_dim(cot_list, cot_out, micro_id, 0)
            return cot_list, acc_first + jnp.swapaxes(grad_first, 0, 1), acc_second + jnp.swapaxes(grad_second, 0, 1)

        cot_stack, acc_first, acc_second = lax.fori_loop(0, STAGES - stage_id, micro_body, (cot_stack, acc_in[stage_id], acc_out[stage_id]))
        mean_first = jnp.sum(acc_first.astype(jnp.bfloat16).astype(jnp.float32), axis=0) / REPLICAS
        mean_second = jnp.sum(acc_second.astype(jnp.bfloat16).astype(jnp.float32), axis=0) / REPLICAS
        grad_in = lax.dynamic_update_index_in_dim(grad_in, mean_first, stage_id, 0)
        grad_out = lax.dynamic_update_index_in_dim(grad_out, mean_second, stage_id, 0)
        return cot_stack, grad_in, grad_out

    start_state = (jnp.zeros((STAGES, ROWS, HIDDEN), jnp.bfloat16), jnp.zeros((STAGES, LAYERS_STAGE, HIDDEN, FF_WIDTH), jnp.float32), jnp.zeros((STAGES, LAYERS_STAGE, FF_WIDTH, HIDDEN), jnp.float32))
    cot_stack, grad_in, grad_out = lax.fori_loop(0, STAGES, stage_body, start_state)
    return grad_in, grad_out, cot_stack
```

```python
import functools
import jax
import jax.numpy as jnp
from jax import lax
from jax.experimental import pallas as pl
from jax.experimental.pallas import tpu as pltpu
from jax.sharding import PartitionSpec as P

SUB = 4
LAG = 3
MESH = pl.DeviceIdType.MESH
ROOT_2_PI = 0.7978845608028654
CUBIC = 0.044715
F32 = jnp.float32
BF16 = jnp.bfloat16


def gelu_value(h):
    p = ROOT_2_PI + (ROOT_2_PI * CUBIC) * (h * h)
    s = 0.5 + 0.5 * jnp.tanh(h * p)
    return h * s


def gelu_slope(h):
    h2 = h * h
    p = ROOT_2_PI + (ROOT_2_PI * CUBIC) * h2
    s = 0.5 + 0.5 * jnp.tanh(h * p)
    a = h * s
    q = 2.0 * ROOT_2_PI + (6.0 * ROOT_2_PI * CUBIC) * h2
    return a, s + (a - a * s) * q


def dot_nt(a, b):
    return lax.dot_general(a, b, (((1,), (1,)), ((), ())), preferred_element_type=F32)


def dot_tn(a, b):
    return lax.dot_general(a, b, (((0,), (0,)), ((), ())), preferred_element_type=F32)


def kernel(layers, blk, w1_hbm, w2_hbm, x_hbm, h_hbm, dy_hbm, acc1_hbm, acc2_hbm,
           gi_hbm, go_hbm, dx_hbm, dh_hbm,
           part, from_sib, rs1_in, rs2_in, full, to_sib,
           w1b, w2b, hb, xb, dhb, a1b, a2b, c_save, c_cur, c_sum, z_in,
           sw1, sw2, sh, sx, sdh_in, sdh_out, sa1, sa2, s_misc,
           sib_send, sib_recv, rs1_send, rs1_recv, rs2_send, rs2_recv,
           ag2_send, ag2_recv, ag1_send, ag1_recv, out_local, out_send, out_recv,
           z_send, z_recv):
    pp = lax.axis_index('pp')
    dp = lax.axis_index('dp')
    core = lax.rem(dp, 2)
    bx = lax.rem(lax.div(dp, 2), 2)
    by = lax.div(dp, 4)
    b1 = bx + core * (by - bx)
    b2 = by + core * (bx - by)
    d1 = 2 + 2 * core
    d2 = 4 - 2 * core
    n1 = dp + (1 - 2 * b1) * d1
    n2 = dp + (1 - 2 * b2) * d2
    sib = dp + 1 - 2 * core
    quarter = 2 * b1 + b2
    first = pp == 0
    chunks = layers * SUB
    rows = blk // SUB

    barrier = pltpu.get_barrier_semaphore()
    for peer in ((pp, sib), (pp, n1), (pp, n2), (1 - pp, dp)):
        pl.semaphore_signal(barrier, inc=1, device_id=peer, device_id_type=MESH)
    pl.semaphore_wait(barrier, 4)

    def load_w(layer, slot):
        return (pltpu.make_async_copy(w1_hbm.at[0, layer], w1b.at[slot], sw1.at[slot]),
                pltpu.make_async_copy(w2_hbm.at[0, layer], w2b.at[slot], sw2.at[slot]))

    def load_h(micro, layer, slot):
        return pltpu.make_async_copy(h_hbm.at[0, micro, layer], hb.at[slot], sh.at[slot])

    def load_x(micro, layer, slot):
        return pltpu.make_async_copy(x_hbm.at[0, micro, layer], xb.at[slot], sx.at[slot])

    def load_rest(layer, slot):
        return (pltpu.make_async_copy(acc1_hbm.at[0, 0, layer], a1b.at[slot], sa1.at[slot]),
                pltpu.make_async_copy(acc2_hbm.at[0, 0, layer], a2b.at[slot], sa2.at[slot]),
                pltpu.make_async_copy(dh_hbm.at[layer], dhb.at[2 + slot], sdh_in.at[slot]),
                load_h(0, layer, 2 + slot), load_x(0, layer, slot))

    def load_second(layer, slot):
        return load_w(layer, slot) + (load_h(1, layer, slot), load_x(1, layer, 2 + slot))

    def save_dh(layer, slot):
        return pltpu.make_async_copy(dhb.at[slot], dh_hbm.at[layer], sdh_out.at[slot])

    def start_grad(step):
        layer, slot = layers - 1 - step, lax.rem(step, 2)
        for copy in load_rest(layer, slot):
            copy.start()

        @pl.when(first)
        def _():
            for copy in load_second(layer, slot):
                copy.start()

    def rs1(k):
        half = 2 * (1 - b1)
        return pltpu.make_async_remote_copy(part.at[k, pl.ds(half, 2)], rs1_in.at[k], rs1_send.at[k], rs1_recv.at[k],
                                            device_id=(pp, n1), device_id_type=MESH)

    def rs2(k):
        return pltpu.make_async_remote_copy(part.at[k, 2 * b1 + 1 - b2], rs2_in.at[k], rs2_send.at[k], rs2_recv.at[k],
                                            device_id=(pp, n2), device_id_type=MESH)

    def ag2(k):
        return pltpu.make_async_remote_copy(full.at[k, quarter], full.at[k, quarter], ag2_send.at[k], ag2_recv.at[k],
                                            device_id=(pp, n2), device_id_type=MESH)

    def ag1(k):
        mine = full.at[k, pl.ds(2 * b1, 2)]
        return pltpu.make_async_remote_copy(mine, mine, ag1_send.at[k], ag1_recv.at[k],
                                            device_id=(pp, n1), device_id_type=MESH)

    def swap(step):
        slot = lax.rem(step, 2)
        return pltpu.make_async_remote_copy(to_sib.at[slot], from_sib.at[pl.ds(step * SUB, SUB)],
                                            sib_send.at[slot], sib_recv.at[step],
                                            device_id=(pp, sib), device_id_type=MESH)

    def emit(k):
        layer = layers - 1 - lax.div(k, SUB)
        row = pl.multiple_of(lax.rem(k, SUB) * rows, rows)

        def send(src, dst):
            pltpu.make_async_copy(src, dst, out_local).start()
            pltpu.make_async_remote_copy(src, dst, out_send, out_recv, device_id=(pp, sib), device_id_type=MESH).start()

        @pl.when(core == 0)
        def _():
            for q in range(4):
                send(full.at[k, q], gi_hbm.at[layer, pl.ds(row, rows), pl.ds(q * blk, blk)])

        @pl.when(core == 1)
        def _():
            for q in range(4):
                send(full.at[k, q], go_hbm.at[layer, pl.ds(q * blk + row, rows), :])

    def pump(i):
        def phase(n, body):
            k = i - n * LAG
            pl.when((k >= 0) & (k < chunks))(lambda: body(k))

        def sum0(k):
            @pl.when(lax.rem(k, SUB) == 0)
            def _():
                swap(lax.div(k, SUB)).wait_recv()
            part[k] = part[k] + from_sib[k]

        def sum1(k):
            rs1(k).wait()
            for j in range(2):
                part[k, 2 * b1 + j] = part[k, 2 * b1 + j] + rs1_in[k, j]

        def sum2(k):
            rs2(k).wait()
            full[k, quarter] = part[k, quarter] + rs2_in[k]

        def done2(k):
            ag2(k).wait()
            ag1(k).start()

        def done1(k):
            ag1(k).wait()
            emit(k)

        phase(2, sum2)
        phase(1, sum1)
        phase(0, sum0)
        phase(3, done2)
        phase(2, lambda k: ag2(k).start())
        phase(1, lambda k: rs2(k).start())
        phase(0, lambda k: rs1(k).start())
        phase(4, done1)

    def cols(f):
        return slice(f * blk, (f + 1) * blk)

    first_c = pltpu.make_async_copy(dy_hbm.at[0], c_cur, s_misc)
    first_c.start()
    for copy in load_w(layers - 1, 0) + (load_h(0, layers - 1, 0),):
        copy.start()
    first_c.wait()

    def chain(c, hs, ws, with_grads):
        total = None
        for f in range(4):
            h = hb[hs, :, cols(f)].astype(F32)
            a, slope = gelu_slope(h)
            d = (dot_nt(c, w2b[ws, cols(f), :]) * slope).astype(BF16)
            with_grads(f, a, d)
            back = dot_nt(d, w1b[ws, :, cols(f)])
            total = back if total is None else total + back
        return (c.astype(F32) + total).astype(BF16)

    def chain_step(i, carry):
        layer, slot = layers - 1 - i, lax.rem(i, 2)
        for copy in load_w(layer, slot) + (load_h(0, layer, slot),):
            copy.wait()

        @pl.when(i + 1 < layers)
        def _():
            for copy in load_w(layer - 1, 1 - slot) + (load_h(0, layer - 1, 1 - slot),):
                copy.start()

        @pl.when(i + 1 == layers)
        def _():
            start_grad(0)

        @pl.when(i >= 2)
        def _():
            save_dh(layer + 2, slot).wait()

        c = c_cur[...]
        c_save[layer] = c

        def keep(f, a, d):
            dhb[slot, :, cols(f)] = d

        c_cur[...] = chain(c, slot, slot, keep)
        save_dh(layer, slot).start()
        return carry

    lax.fori_loop(0, layers, chain_step, 0)

    down = pltpu.make_async_remote_copy(c_cur, z_in, z_send, z_recv, device_id=(1 - pp, dp), device_id_type=MESH)
    keep_dx = pltpu.make_async_copy(c_cur, dx_hbm, s_misc)

    @pl.when(pp == 1)
    def _():
        down.start()
        down.wait_send()

    @pl.when(first)
    def _():
        keep_dx.start()
        keep_dx.wait()
        down.wait_recv()
        c_cur[...] = z_in[...]

    save_dh(1, lax.rem(layers, 2)).wait()
    save_dh(0, lax.rem(layers + 1, 2)).wait()

    def grad_step(i, carry):
        layer, slot = layers - 1 - i, lax.rem(i, 2)
        for copy in load_rest(layer, slot):
            copy.wait()

        @pl.when(first)
        def _():
            for copy in load_second(layer, slot):
                copy.wait()

        @pl.when(i + 1 < layers)
        def _():
            start_grad(i + 1)

        @pl.when(i >= 2)
        def _():
            swap(i - 2).wait_send()

        x0 = xb[slot]
        c0 = c_save[layer]
        for f in range(4):
            a = gelu_value(hb[2 + slot, :, cols(f)].astype(F32)).astype(BF16)
            a1b[slot, :, cols(f)] += dot_tn(x0, dhb[2 + slot, :, cols(f)])
            a2b[slot, cols(f), :] += dot_tn(a, c0)

        pump(2 * i - 1)

        @pl.when(first)
        def _():
            c = c_cur[...]
            x1 = xb[2 + slot]

            def add(f, a, d):
                a1b[slot, :, cols(f)] += dot_tn(x1, d)
                a2b[slot, cols(f), :] += dot_tn(a.astype(BF16), c)

            c_cur[...] = chain(c, slot, slot, add)

        for f in range(4):
            g1 = a1b[slot, :, cols(f)].astype(BF16)
            g2 = a2b[slot, cols(f), :].astype(BF16)
            own = jnp.where(core == 0, g1, g2)
            other = jnp.where(core == 0, g2, g1)
            for s in range(SUB):
                part[i * SUB + s, f] = own[s * rows:(s + 1) * rows]
                to_sib[slot, s, f] = other[s * rows:(s + 1) * rows]
        swap(i).start()
        pump(2 * i)
        return carry

    lax.fori_loop(0, layers, grad_step, 0)

    @pl.when(first)
    def _():
        down.start()

    for i in (layers - 2, layers - 1):
        swap(i).wait_send()

    def tail_step(i, carry):
        pump(i)
        return carry

    lax.fori_loop(2 * layers - 1, chunks + 4 * LAG, tail_step, 0)

    @pl.when(first)
    def _():
        down.wait_send()

    @pl.when(pp == 1)
    def _():
        down.wait_recv()
        put = pltpu.make_async_copy(z_in, dx_hbm, s_misc)
        put.start()
        put.wait()

    pltpu.make_async_copy(gi_hbm, gi_hbm, out_local).wait()
    pltpu.make_async_copy(gi_hbm, gi_hbm, out_send).wait()
    pltpu.make_async_copy(go_hbm, go_hbm, out_recv).wait()


def solution(mesh):
    replicas = mesh.shape['dp']

    def device_fn(w_in, w_out, x_saved, h_saved, dy_in, acc_in, acc_out):
        layers, hidden, ff = w_in.shape[1:]
        tokens = dy_in.shape[1]
        blk = ff // 4
        chunks, rows = layers * SUB, blk // SUB
        dma = pltpu.SemaphoreType.DMA
        flops = 2 * tokens * hidden * ff * layers * 8
        call = pl.pallas_call(
            functools.partial(kernel, layers, blk),
            out_shape=(
                jax.ShapeDtypeStruct((layers, hidden, ff), BF16),
                jax.ShapeDtypeStruct((layers, ff, hidden), BF16),
                jax.ShapeDtypeStruct((tokens, hidden), BF16),
                jax.ShapeDtypeStruct((layers, tokens, ff), BF16),
            ),
            in_specs=[pl.BlockSpec(memory_space=pl.ANY)] * 7,
            out_specs=[pl.BlockSpec(memory_space=pl.ANY)] * 4,
            scratch_shapes=[
                pltpu.VMEM((chunks, 4, rows, hidden), BF16),
                pltpu.VMEM((chunks, 4, rows, hidden), BF16),
                pltpu.VMEM((chunks, 2, rows, hidden), BF16),
                pltpu.VMEM((chunks, rows, hidden), BF16),
                pltpu.VMEM((chunks, 4, rows, hidden), BF16),
                pltpu.VMEM((2, SUB, 4, rows, hidden), BF16),
                pltpu.VMEM((2, hidden, ff), BF16),
                pltpu.VMEM((2, ff, hidden), BF16),
                pltpu.VMEM((4, tokens, ff), BF16),
                pltpu.VMEM((4, tokens, hidden), BF16),
                pltpu.VMEM((4, tokens, ff), BF16),
                pltpu.VMEM((2, hidden, ff), F32),
                pltpu.VMEM((2, ff, hidden), F32),
                pltpu.VMEM((layers, tokens, hidden), BF16),
                pltpu.VMEM((tokens, hidden), BF16),
                pltpu.VMEM((8, 128), F32),
                pltpu.VMEM((tokens, hidden), BF16),
                dma((2,)), dma((2,)), dma((4,)), dma((4,)), dma((2,)), dma((2,)), dma((2,)), dma((2,)), dma,
                dma((2,)), dma((layers,)),
                dma((chunks,)), dma((chunks,)), dma((chunks,)), dma((chunks,)),
                dma((chunks,)), dma((chunks,)), dma((chunks,)), dma((chunks,)),
                dma, dma, dma, dma, dma,
            ],
            compiler_params=pltpu.CompilerParams(collective_id=0, has_side_effects=True, vmem_limit_bytes=67043328),
            cost_estimate=pl.CostEstimate(flops=flops, bytes_accessed=200 << 20, transcendentals=0),
        )
        grad_in, grad_out, dx_out, _ = call(w_in, w_out, x_saved, h_saved, dy_in, acc_in, acc_out)
        scale = 1.0 / replicas
        return (grad_in.astype(F32) * scale)[None], (grad_out.astype(F32) * scale)[None], dx_out[None]

    return jax.shard_map(device_fn, mesh=mesh, in_specs=(P('pp'), P('pp'), P('pp', None, None, 'dp'), P('pp', None, None, 'dp'), P('pp', 'dp'), P('pp', 'dp'), P('pp', 'dp')), out_specs=(P('pp'), P('pp'), P('pp', 'dp')), check_vma=False)
```

```python
import functools
import jax
import jax.numpy as jnp
from jax import lax
from jax.experimental import pallas as pl
from jax.experimental.pallas import tpu as pltpu
from jax.sharding import PartitionSpec as P

SUB = 2
LAG = 3
RING = 8
MESH = pl.DeviceIdType.MESH
ROOT_2_PI = 0.7978845608028654
CUBIC = 0.044715
F32 = jnp.float32
BF16 = jnp.bfloat16


def gelu_value(h):
    p = ROOT_2_PI + (ROOT_2_PI * CUBIC) * (h * h)
    s = 0.5 + 0.5 * jnp.tanh(h * p)
    return h * s


def gelu_slope(h):
    h2 = h * h
    p = ROOT_2_PI + (ROOT_2_PI * CUBIC) * h2
    s = 0.5 + 0.5 * jnp.tanh(h * p)
    a = h * s
    q = 2.0 * ROOT_2_PI + (6.0 * ROOT_2_PI * CUBIC) * h2
    return a, s + (a - a * s) * q


def dot_nt(a, b):
    return lax.dot_general(a, b, (((1,), (1,)), ((), ())), preferred_element_type=F32)


def dot_tn(a, b):
    return lax.dot_general(a, b, (((0,), (0,)), ((), ())), preferred_element_type=F32)


def kernel(layers, blk, w1_hbm, w2_hbm, x_hbm, h_hbm, dy_hbm, acc1_hbm, acc2_hbm,
           full, other, dx, dh_hbm,
           part, from_sib, rs1_in, rs2_in, to_sib,
           w1b, w2b, hb, xb, dhb, a1b, a2b, c_save, c_cur, z_in,
           sw1, sw2, sh, sx, sdh_in, sdh_out, sa1, sa2, s_misc,
           sib_send, sib_recv, rs1_send, rs1_recv, rs2_send, rs2_recv,
           ag2_send, ag2_recv, ag1_send, ag1_recv, out_send, out_recv,
           z_send, z_recv):
    pp = lax.axis_index('pp')
    dp = lax.axis_index('dp')
    core = lax.rem(dp, 2)
    bx = lax.rem(lax.div(dp, 2), 2)
    by = lax.div(dp, 4)
    b1 = bx + core * (by - bx)
    b2 = by + core * (bx - by)
    d1 = 2 + 2 * core
    d2 = 4 - 2 * core
    n1 = dp + (1 - 2 * b1) * d1
    n2 = dp + (1 - 2 * b2) * d2
    sib = dp + 1 - 2 * core
    quarter = 2 * b1 + b2
    first = pp == 0
    chunks = layers * SUB
    rows = blk // SUB

    barrier = pltpu.get_barrier_semaphore()
    for peer in ((pp, sib), (pp, n1), (pp, n2), (1 - pp, dp)):
        pl.semaphore_signal(barrier, inc=1, device_id=peer, device_id_type=MESH)
    pl.semaphore_wait(barrier, 4)

    def load_w(layer, slot):
        return (pltpu.make_async_copy(w1_hbm.at[0, layer], w1b.at[slot], sw1.at[slot]),
                pltpu.make_async_copy(w2_hbm.at[0, layer], w2b.at[slot], sw2.at[slot]))

    def load_h(micro, layer, slot):
        return pltpu.make_async_copy(h_hbm.at[0, micro, layer], hb.at[slot], sh.at[slot])

    def load_x(micro, layer, slot):
        return pltpu.make_async_copy(x_hbm.at[0, micro, layer], xb.at[slot], sx.at[slot])

    def load_rest(layer, slot):
        return (pltpu.make_async_copy(acc1_hbm.at[0, 0, layer], a1b.at[slot], sa1.at[slot]),
                pltpu.make_async_copy(acc2_hbm.at[0, 0, layer], a2b.at[slot], sa2.at[slot]),
                pltpu.make_async_copy(dh_hbm.at[layer], dhb.at[2 + slot], sdh_in.at[slot]),
                load_h(0, layer, 2 + slot), load_x(0, layer, slot))

    def load_second(layer, slot):
        return load_w(layer, slot) + (load_h(1, layer, slot), load_x(1, layer, 2 + slot))

    def save_dh(layer, slot):
        return pltpu.make_async_copy(dhb.at[slot], dh_hbm.at[layer], sdh_out.at[slot])

    def start_grad(step):
        layer, slot = layers - 1 - step, lax.rem(step, 2)
        for copy in load_rest(layer, slot):
            copy.start()

        @pl.when(first)
        def _():
            for copy in load_second(layer, slot):
                copy.start()

    def rs1(k):
        half = 2 * (1 - b1)
        return pltpu.make_async_remote_copy(part.at[k, pl.ds(half, 2)], rs1_in.at[k], rs1_send.at[lax.rem(k, RING)], rs1_recv.at[lax.rem(k, RING)],
                                            device_id=(pp, n1), device_id_type=MESH)

    def rs2(k):
        return pltpu.make_async_remote_copy(part.at[k, 2 * b1 + 1 - b2], rs2_in.at[k], rs2_send.at[lax.rem(k, RING)], rs2_recv.at[lax.rem(k, RING)],
                                            device_id=(pp, n2), device_id_type=MESH)

    def ag2(k):
        return pltpu.make_async_remote_copy(full.at[k, quarter], full.at[k, quarter], ag2_send.at[lax.rem(k, RING)], ag2_recv.at[lax.rem(k, RING)],
                                            device_id=(pp, n2), device_id_type=MESH)

    def ag1(k):
        mine = full.at[k, pl.ds(2 * b1, 2)]
        return pltpu.make_async_remote_copy(mine, mine, ag1_send.at[lax.rem(k, RING)], ag1_recv.at[lax.rem(k, RING)],
                                            device_id=(pp, n1), device_id_type=MESH)

    def swap(step):
        slot = lax.rem(step, 2)
        return pltpu.make_async_remote_copy(to_sib.at[slot], from_sib.at[pl.ds(step * SUB, SUB)],
                                            sib_send.at[slot], sib_recv.at[step],
                                            device_id=(pp, sib), device_id_type=MESH)

    def emit(k):
        pltpu.make_async_remote_copy(full.at[k], other.at[k], out_send, out_recv,
                                     device_id=(pp, sib), device_id_type=MESH).start()

    def pump(i):
        def phase(n, body):
            k = i - n * LAG
            pl.when((k >= 0) & (k < chunks))(lambda: body(k))

        def sum0(k):
            @pl.when(lax.rem(k, SUB) == 0)
            def _():
                swap(lax.div(k, SUB)).wait_recv()
            part[k] = part[k] + from_sib[k]

        def sum1(k):
            rs1(k).wait()
            for j in range(2):
                part[k, 2 * b1 + j] = part[k, 2 * b1 + j] + rs1_in[k, j]

        def sum2(k):
            rs2(k).wait()
            full[k, quarter] = part[k, quarter] + rs2_in[k]

        def done2(k):
            ag2(k).wait()
            ag1(k).start()

        def done1(k):
            ag1(k).wait()
            emit(k)

        phase(2, sum2)
        phase(1, sum1)
        phase(0, sum0)
        phase(3, done2)
        phase(2, lambda k: ag2(k).start())
        phase(1, lambda k: rs2(k).start())
        phase(0, lambda k: rs1(k).start())
        phase(4, done1)

    def cols(f):
        return slice(f * blk, (f + 1) * blk)

    first_c = pltpu.make_async_copy(dy_hbm.at[0], c_cur, s_misc)
    first_c.start()
    for copy in load_w(layers - 1, 0) + (load_h(0, layers - 1, 0),):
        copy.start()
    first_c.wait()

    def chain(c, hs, ws, with_grads):
        total = None
        for f in range(4):
            h = hb[hs, :, cols(f)].astype(F32)
            a, slope = gelu_slope(h)
            d = (dot_nt(c, w2b[ws, cols(f), :]) * slope).astype(BF16)
            with_grads(f, a, d)
            back = dot_nt(d, w1b[ws, :, cols(f)])
            total = back if total is None else total + back
        return (c.astype(F32) + total).astype(BF16)

    def chain_step(i, carry):
        layer, slot = layers - 1 - i, lax.rem(i, 2)
        for copy in load_w(layer, slot) + (load_h(0, layer, slot),):
            copy.wait()

        @pl.when(i + 1 < layers)
        def _():
            for copy in load_w(layer - 1, 1 - slot) + (load_h(0, layer - 1, 1 - slot),):
                copy.start()

        @pl.when(i + 1 == layers)
        def _():
            start_grad(0)

        @pl.when(i >= 2)
        def _():
            save_dh(layer + 2, slot).wait()

        c = c_cur[...]
        c_save[layer] = c

        def keep(f, a, d):
            dhb[slot, :, cols(f)] = d

        c_cur[...] = chain(c, slot, slot, keep)
        save_dh(layer, slot).start()
        return carry

    lax.fori_loop(0, layers, chain_step, 0)

    down = pltpu.make_async_remote_copy(c_cur, z_in, z_send, z_recv, device_id=(1 - pp, dp), device_id_type=MESH)

    @pl.when(pp == 1)
    def _():
        down.start()
        down.wait_send()

    @pl.when(first)
    def _():
        dx[...] = c_cur[...]

    save_dh(1, lax.rem(layers, 2)).wait()
    save_dh(0, lax.rem(layers + 1, 2)).wait()

    def grad_step(i, carry):
        layer, slot = layers - 1 - i, lax.rem(i, 2)
        for copy in load_rest(layer, slot):
            copy.wait()

        @pl.when(first)
        def _():
            for copy in load_second(layer, slot):
                copy.wait()

        @pl.when(i + 1 < layers)
        def _():
            start_grad(i + 1)

        @pl.when(i >= 2)
        def _():
            swap(i - 2).wait_send()

        x0 = xb[slot]
        c0 = c_save[layer]
        for f in range(4):
            a = gelu_value(hb[2 + slot, :, cols(f)].astype(F32)).astype(BF16)
            a1b[slot, :, cols(f)] += dot_tn(x0, dhb[2 + slot, :, cols(f)])
            a2b[slot, cols(f), :] += dot_tn(a, c0)

        pump(2 * i - 1)

        @pl.when(first)
        def _():
            @pl.when(i == 0)
            def _():
                down.wait_recv()
                c_cur[...] = z_in[...]

            c = c_cur[...]
            x1 = xb[2 + slot]

            def add(f, a, d):
                a1b[slot, :, cols(f)] += dot_tn(x1, d)
                a2b[slot, cols(f), :] += dot_tn(a.astype(BF16), c)

            c_cur[...] = chain(c, slot, slot, add)

        for f in range(4):
            g1 = a1b[slot, :, cols(f)].astype(BF16)
            g2 = a2b[slot, cols(f), :].astype(BF16)
            own = jnp.where(core == 0, g1, g2)
            other = jnp.where(core == 0, g2, g1)
            for s in range(SUB):
                part[i * SUB + s, f] = own[s * rows:(s + 1) * rows]
                to_sib[slot, s, f] = other[s * rows:(s + 1) * rows]
        swap(i).start()
        pump(2 * i)
        return carry

    lax.fori_loop(0, layers, grad_step, 0)

    @pl.when(first)
    def _():
        down.start()

    for i in (layers - 2, layers - 1):
        swap(i).wait_send()

    def tail_step(i, carry):
        pump(i)
        return carry

    lax.fori_loop(2 * layers - 1, chunks + 4 * LAG, tail_step, 0)

    @pl.when(first)
    def _():
        down.wait_send()

    @pl.when(pp == 1)
    def _():
        down.wait_recv()
        dx[...] = z_in[...]

    pltpu.make_async_copy(full, full, out_send).wait()
    pltpu.make_async_copy(other, other, out_recv).wait()


def widen(layers, blk, scale, own, other, dx, gi_hbm, go_hbm, dx_hbm, gi_buf, go_buf, gi_sem, go_sem, dx_sem):
    put_dx = pltpu.make_async_copy(dx, dx_hbm, dx_sem)
    put_dx.start()
    core = lax.rem(lax.axis_index('dp'), 2)
    rows = blk // SUB

    def step(i, carry):
        layer, slot = layers - 1 - i, lax.rem(i, 2)
        puts = (pltpu.make_async_copy(gi_buf.at[slot], gi_hbm.at[layer], gi_sem.at[slot]),
                pltpu.make_async_copy(go_buf.at[slot], go_hbm.at[layer], go_sem.at[slot]))

        @pl.when(i >= 2)
        def _():
            for put in puts:
                put.wait()

        def fill(gi, go):
            for q in range(4):
                for s in range(SUB):
                    r = slice(s * rows, (s + 1) * rows)
                    gi_buf[slot, r, q * blk:(q + 1) * blk] = gi[i * SUB + s, q].astype(F32) * scale
                    go_buf[slot, q * blk + s * rows:q * blk + (s + 1) * rows, :] = go[i * SUB + s, q].astype(F32) * scale

        pl.when(core == 0)(lambda: fill(own, other))
        pl.when(core == 1)(lambda: fill(other, own))
        for put in puts:
            put.start()
        return carry

    lax.fori_loop(0, layers, step, 0)
    for slot in range(2):
        pltpu.make_async_copy(gi_buf.at[slot], gi_hbm.at[slot], gi_sem.at[slot]).wait()
        pltpu.make_async_copy(go_buf.at[slot], go_hbm.at[slot], go_sem.at[slot]).wait()
    put_dx.wait()


def solution(mesh):
    replicas = mesh.shape['dp']

    def device_fn(w_in, w_out, x_saved, h_saved, dy_in, acc_in, acc_out):
        layers, hidden, ff = w_in.shape[1:]
        tokens = dy_in.shape[1]
        blk = ff // 4
        chunks, rows = layers * SUB, blk // SUB
        dma = pltpu.SemaphoreType.DMA
        flops = 2 * tokens * hidden * ff * layers * 8
        call = pl.pallas_call(
            functools.partial(kernel, layers, blk),
            out_shape=(
                pltpu.VMEM((chunks, 4, rows, hidden), BF16),
                pltpu.VMEM((chunks, 4, rows, hidden), BF16),
                pltpu.VMEM((tokens, hidden), BF16),
                jax.ShapeDtypeStruct((layers, tokens, ff), BF16),
            ),
            in_specs=[pl.BlockSpec(memory_space=pl.ANY)] * 7,
            out_specs=[pl.BlockSpec(memory_space=pltpu.VMEM)] * 3 + [pl.BlockSpec(memory_space=pl.ANY)],
            scratch_shapes=[
                pltpu.VMEM((chunks, 4, rows, hidden), BF16),
                pltpu.VMEM((chunks, 4, rows, hidden), BF16),
                pltpu.VMEM((chunks, 2, rows, hidden), BF16),
                pltpu.VMEM((chunks, rows, hidden), BF16),
                pltpu.VMEM((2, SUB, 4, rows, hidden), BF16),
                pltpu.VMEM((2, hidden, ff), BF16),
                pltpu.VMEM((2, ff, hidden), BF16),
                pltpu.VMEM((4, tokens, ff), BF16),
                pltpu.VMEM((4, tokens, hidden), BF16),
                pltpu.VMEM((4, tokens, ff), BF16),
                pltpu.VMEM((2, hidden, ff), F32),
                pltpu.VMEM((2, ff, hidden), F32),
                pltpu.VMEM((layers, tokens, hidden), BF16),
                pltpu.VMEM((tokens, hidden), BF16),
                pltpu.VMEM((tokens, hidden), BF16),
                dma((2,)), dma((2,)), dma((4,)), dma((4,)), dma((2,)), dma((2,)), dma((2,)), dma((2,)), dma,
                dma((2,)), dma((layers,)),
                dma((RING,)), dma((RING,)), dma((RING,)), dma((RING,)),
                dma((RING,)), dma((RING,)), dma((RING,)), dma((RING,)),
                dma, dma, dma, dma,
            ],
            compiler_params=pltpu.CompilerParams(collective_id=0, has_side_effects=True, vmem_limit_bytes=67043328 - (33 << 19)),
            cost_estimate=pl.CostEstimate(flops=flops, bytes_accessed=200 << 20, transcendentals=0),
        )
        own, other, dx, _ = call(w_in, w_out, x_saved, h_saved, dy_in, acc_in, acc_out)
        grad_in, grad_out, dx_out = pl.pallas_call(
            functools.partial(widen, layers, blk, 1.0 / replicas),
            out_shape=(jax.ShapeDtypeStruct((layers, hidden, ff), F32), jax.ShapeDtypeStruct((layers, ff, hidden), F32),
                       jax.ShapeDtypeStruct((tokens, hidden), BF16)),
            in_specs=[pl.BlockSpec(memory_space=pltpu.VMEM)] * 3,
            out_specs=[pl.BlockSpec(memory_space=pl.ANY)] * 3,
            scratch_shapes=[pltpu.VMEM((2, hidden, ff), F32), pltpu.VMEM((2, ff, hidden), F32), dma((2,)), dma((2,)), dma],
            compiler_params=pltpu.CompilerParams(vmem_limit_bytes=12 << 20),
        )(own, other, dx)
        return grad_in[None], grad_out[None], dx_out[None]

    return jax.shard_map(device_fn, mesh=mesh, in_specs=(P('pp'), P('pp'), P('pp', None, None, 'dp'), P('pp', None, None, 'dp'), P('pp', 'dp'), P('pp', 'dp'), P('pp', 'dp')), out_specs=(P('pp'), P('pp'), P('pp', 'dp')), check_vma=False)
```

```python
import functools
import jax
import jax.numpy as jnp
from jax import lax
from jax.experimental import pallas as pl
from jax.experimental.pallas import tpu as pltpu
from jax.sharding import PartitionSpec as P

SUB = 2
LAG = 3
RING = 8
DEPTH = 4
EARLY = 3
GAP = 5
LENDS = (4, 8)
LENT = len(LENDS)
TAKE_AT = 12
MESH = pl.DeviceIdType.MESH
ROOT_2_PI = 0.7978845608028654
CUBIC = 0.044715
F32 = jnp.float32
BF16 = jnp.bfloat16


def gelu_value(h):
    p = ROOT_2_PI + (ROOT_2_PI * CUBIC) * (h * h)
    s = 0.5 + 0.5 * jnp.tanh(h * p)
    return h * s


def gelu_slope(h):
    h2 = h * h
    p = ROOT_2_PI + (ROOT_2_PI * CUBIC) * h2
    s = 0.5 + 0.5 * jnp.tanh(h * p)
    a = h * s
    q = 2.0 * ROOT_2_PI + (6.0 * ROOT_2_PI * CUBIC) * h2
    return a, s + (a - a * s) * q


def dot_nt(a, b):
    return lax.dot_general(a, b, (((1,), (1,)), ((), ())), preferred_element_type=F32)


def dot_tn(a, b):
    return lax.dot_general(a, b, (((0,), (0,)), ((), ())), preferred_element_type=F32)


def layer_of(pp, made, layers):
    j = made - EARLY
    late = jnp.minimum(j + 1 + lax.div(j, GAP - 1), layers - 1)
    early = (made < EARLY).astype(jnp.int32)
    return layers - 1 - (made + pp * (late + early * (GAP * made - late) - made))


def kernel(layers, blk, w1_hbm, w2_hbm, x_hbm, h_hbm, dy_hbm, acc1_hbm, acc2_hbm,
           full, other, dx, dh_hbm,
           part, from_sib, rs1_in, rs2_in, to_sib,
           w1b, w2b, hb, xb, dhb, a1b, a2b, c_save, c_cur, z_in,
           sw1, sw2, sh, sx, sdh_in, sdh_out, sa1, sa2, s_misc,
           sib_send, sib_recv, rs1_send, rs1_recv, rs2_send, rs2_recv,
           ag2_send, ag2_recv, ag1_send, ag1_recv, out_send, out_recv,
           z_send, z_recv,
           lend_send, lend_recv, back_send, back_recv, sib_free):
    pp = lax.axis_index('pp')
    dp = lax.axis_index('dp')
    core = lax.rem(dp, 2)
    bx = lax.rem(lax.div(dp, 2), 2)
    by = lax.div(dp, 4)
    b1 = bx + core * (by - bx)
    b2 = by + core * (bx - by)
    d1 = 2 + 2 * core
    d2 = 4 - 2 * core
    n1 = dp + (1 - 2 * b1) * d1
    n2 = dp + (1 - 2 * b2) * d2
    sib = dp + 1 - 2 * core
    quarter = 2 * b1 + b2
    first = pp == 0
    taken = pp * LENT
    chunks = (layers - LENT + 2 * taken) * SUB
    rows = blk // SUB

    def load_w(layer, slot):
        return (pltpu.make_async_copy(w1_hbm.at[0, layer], w1b.at[slot], sw1.at[slot]),
                pltpu.make_async_copy(w2_hbm.at[0, layer], w2b.at[slot], sw2.at[slot]))

    def load_h(micro, layer, slot):
        return pltpu.make_async_copy(h_hbm.at[0, micro, layer], hb.at[slot], sh.at[slot])

    def load_x(micro, layer, slot):
        return pltpu.make_async_copy(x_hbm.at[0, micro, layer], xb.at[slot], sx.at[slot])

    def load_sums(layer, slot):
        return (pltpu.make_async_copy(acc1_hbm.at[0, 0, layer], a1b.at[slot], sa1.at[slot]),
                pltpu.make_async_copy(acc2_hbm.at[0, 0, layer], a2b.at[slot], sa2.at[slot]),
                load_x(0, layer, slot))

    def load_rest(layer, slot):
        return load_sums(layer, slot) + (
            pltpu.make_async_copy(dh_hbm.at[layer], dhb.at[2 + slot], sdh_in.at[slot]),
            load_h(0, layer, 2 + slot))

    def load_second(layer, slot):
        return load_w(layer, slot) + (load_h(1, layer, slot), load_x(1, layer, 2 + slot))

    def save_dh(layer, slot):
        return pltpu.make_async_copy(dhb.at[slot], dh_hbm.at[layer], sdh_out.at[slot])

    def start_grad(step):
        layer, slot = layer_of(pp, step + EARLY * pp, layers), lax.rem(step, 2)
        for copy in load_rest(layer, slot):
            copy.start()

        @pl.when(first)
        def _():
            for copy in load_second(layer, slot):
                copy.start()

    def place(k):
        p, sub = lax.div(k, SUB), lax.rem(k, SUB)
        late = sum((p >= m - n).astype(jnp.int32) for n, m in enumerate(LENDS))
        after = (p >= TAKE_AT).astype(jnp.int32)
        past = (p >= TAKE_AT + LENT).astype(jnp.int32)
        zero = p + late
        one = p + (layers - TAKE_AT) * (after - past) - LENT * past
        return (zero + pp * (one - zero)) * SUB + sub

    def remote(src, dst, send, recv, peer):
        return pltpu.make_async_remote_copy(src, dst, send, recv, device_id=peer, device_id_type=MESH)

    def rs1(k):
        b, r = place(k), lax.rem(k, RING)
        return remote(part.at[b, pl.ds(2 * (1 - b1), 2)], rs1_in.at[b], rs1_send.at[r], rs1_recv.at[r], (pp, n1))

    def rs2(k):
        b, r = place(k), lax.rem(k, RING)
        return remote(part.at[b, 2 * b1 + 1 - b2], rs2_in.at[b], rs2_send.at[r], rs2_recv.at[r], (pp, n2))

    def ag2(k):
        b, r = place(k), lax.rem(k, RING)
        return remote(full.at[b, quarter], full.at[b, quarter], ag2_send.at[r], ag2_recv.at[r], (pp, n2))

    def ag1(k):
        b, r = place(k), lax.rem(k, RING)
        mine = full.at[b, pl.ds(2 * b1, 2)]
        return remote(mine, mine, ag1_send.at[r], ag1_recv.at[r], (pp, n1))

    def swap(made):
        slot, held = lax.rem(made, 2), lax.rem(made, DEPTH)
        return remote(to_sib.at[slot], from_sib.at[held], sib_send.at[slot], sib_recv.at[held], (pp, sib))

    def freed(made):
        @pl.when(made + DEPTH < layers)
        def _():
            pl.semaphore_signal(sib_free, inc=1, device_id=(pp, sib), device_id_type=MESH)

    def lend(n):
        return remote(part.at[pl.ds(LENDS[n] * SUB, SUB)], part.at[pl.ds((layers + n) * SUB, SUB)],
                      lend_send.at[n], lend_recv.at[n], (1 - pp, dp))

    def give_back(n):
        return remote(full.at[layers * SUB + n], full.at[LENDS[n // SUB] * SUB + n % SUB],
                      back_send.at[n], back_recv.at[n], (1 - pp, dp))

    def emit(b):
        remote(full.at[b], other.at[b], out_send, out_recv, (pp, sib)).start()

    def lend_out(n):
        made = LENDS[n]
        swap(made).wait_recv()
        for t in range(SUB):
            part[made * SUB + t] = part[made * SUB + t] + from_sib[made % DEPTH, t]
        freed(made)
        lend(n).start()

    def chunk_at(step):
        turn, at = lax.div(step, GAP), lax.rem(step, GAP)
        chain = (step < layers).astype(jnp.int32)
        one = (1 - chain) * (step - layers + EARLY * SUB) + chain * (2 * turn + lax.div(at, 2))
        k = step + pp * (one - step)
        idle = (pp == 1) & (step < layers) & ((turn >= EARLY) | ((at != 1) & (at != 3)))
        return k, (step >= 0) & (k < chunks) & jnp.logical_not(idle)

    def pump(i):
        def phase(n, body):
            k, there = chunk_at(i - n * LAG)
            pl.when(there)(lambda: body(k))

        def sum0(k):
            b, sub = place(k), lax.rem(k, SUB)
            made = lax.div(b, SUB)

            @pl.when(made < layers)
            def _():
                @pl.when(sub == 0)
                def _():
                    swap(made).wait_recv()
                part[b] = part[b] + from_sib[lax.rem(made, DEPTH), sub]

                @pl.when(sub == SUB - 1)
                def _():
                    freed(made)

            for n in range(LENT):
                @pl.when((made == layers + n) & (sub == 0))
                def _():
                    lend(n).wait_recv()

        def sum1(k):
            rs1(k).wait()
            b = place(k)
            for j in range(2):
                part[b, 2 * b1 + j] = part[b, 2 * b1 + j] + rs1_in[b, j]

        def sum2(k):
            rs2(k).wait()
            b = place(k)
            full[b, quarter] = part[b, quarter] + rs2_in[b]

        def done2(k):
            ag2(k).wait()
            ag1(k).start()

        def done1(k):
            ag1(k).wait()
            b = place(k)
            pl.when(b < layers * SUB)(lambda: emit(b))
            for n in range(LENT * SUB):
                pl.when(b == layers * SUB + n)(lambda n=n: give_back(n).start())

        phase(2, sum2)
        phase(1, sum1)
        phase(0, sum0)
        phase(3, done2)
        phase(2, lambda k: ag2(k).start())
        phase(1, lambda k: rs2(k).start())
        phase(0, lambda k: rs1(k).start())
        phase(4, done1)

    def cols(f):
        return slice(f * blk, (f + 1) * blk)

    first_c = pltpu.make_async_copy(dy_hbm.at[0], c_cur, s_misc)
    first_c.start()
    for copy in load_w(layers - 1, 0) + (load_h(0, layers - 1, 0),):
        copy.start()
    @pl.when(pp == 1)
    def _():
        for copy in load_sums(layers - 1, 0):
            copy.start()

    barrier = pltpu.get_barrier_semaphore()
    for peer in ((pp, sib), (pp, n1), (pp, n2), (1 - pp, dp)):
        pl.semaphore_signal(barrier, inc=1, device_id=peer, device_id_type=MESH)
    pl.semaphore_wait(barrier, 4)
    first_c.wait()

    def chain(c, hs, ws, with_grads):
        total = None
        for f in range(4):
            h = hb[hs, :, cols(f)].astype(F32)
            a, slope = gelu_slope(h)
            d = (dot_nt(c, w2b[ws, cols(f), :]) * slope).astype(BF16)
            with_grads(f, a, d)
            back = dot_nt(d, w1b[ws, :, cols(f)])
            total = back if total is None else total + back
        return (c.astype(F32) + total).astype(BF16)

    def first_grads(layer, slot, hs, ds):
        x0 = xb[slot]
        c0 = c_save[layer]
        for f in range(4):
            a = gelu_value(hb[hs, :, cols(f)].astype(F32)).astype(BF16)
            a1b[slot, :, cols(f)] += dot_tn(x0, dhb[ds, :, cols(f)])
            a2b[slot, cols(f), :] += dot_tn(a, c0)

    def publish(made, slot):
        @pl.when(made >= 2)
        def _():
            swap(made - 2).wait_send()

        for f in range(4):
            g1 = a1b[slot, :, cols(f)].astype(BF16)
            g2 = a2b[slot, cols(f), :].astype(BF16)
            own = jnp.where(core == 0, g1, g2)
            rest = jnp.where(core == 0, g2, g1)
            for t in range(SUB):
                part[made * SUB + t, f] = own[t * rows:(t + 1) * rows]
                to_sib[lax.rem(made, 2), t, f] = rest[t * rows:(t + 1) * rows]

        @pl.when(made >= DEPTH)
        def _():
            pl.semaphore_wait(sib_free, 1)
        swap(made).start()

    def chain_step(i, carry):
        layer, slot = layers - 1 - i, lax.rem(i, 2)
        for copy in load_w(layer, slot) + (load_h(0, layer, slot),):
            copy.wait()

        @pl.when(i + 1 < layers)
        def _():
            for copy in load_w(layer - 1, 1 - slot) + (load_h(0, layer - 1, 1 - slot),):
                copy.start()

        @pl.when(i + 1 == layers)
        def _():
            start_grad(0)

        @pl.when(i >= 2)
        def _():
            save_dh(layer + 2, slot).wait()

        c = c_cur[...]
        c_save[layer] = c

        def keep(f, a, d):
            dhb[slot, :, cols(f)] = d

        c_cur[...] = chain(c, slot, slot, keep)
        save_dh(layer, slot).start()

        turn, at = lax.div(i, GAP), lax.rem(i, GAP)

        @pl.when((pp == 1) & (at == 0) & (turn < EARLY))
        def _():
            held = lax.rem(turn, 2)
            for copy in load_sums(layer, held):
                copy.wait()

            @pl.when(turn + 1 < EARLY)
            def _():
                for copy in load_sums(layer - GAP, 1 - held):
                    copy.start()

            first_grads(layer, held, slot, slot)
            publish(turn, held)

        @pl.when(pp == 1)
        def _():
            pump(i)
        return carry

    lax.fori_loop(0, layers, chain_step, 0)

    down = pltpu.make_async_remote_copy(c_cur, z_in, z_send, z_recv, device_id=(1 - pp, dp), device_id_type=MESH)

    @pl.when(pp == 1)
    def _():
        down.start()

    @pl.when(first)
    def _():
        dx[...] = c_cur[...]

    save_dh(1, lax.rem(layers, 2)).wait()
    save_dh(0, lax.rem(layers + 1, 2)).wait()

    def grad_step(i, carry):
        made = i + EARLY * pp
        layer, slot = layer_of(pp, made, layers), lax.rem(i, 2)
        for copy in load_rest(layer, slot):
            copy.wait()

        @pl.when(first)
        def _():
            for copy in load_second(layer, slot):
                copy.wait()

        @pl.when(made + 1 < layers)
        def _():
            start_grad(i + 1)

        first_grads(layer, slot, 2 + slot, 2 + slot)

        lent = sum((made > m).astype(jnp.int32) for m in LENDS)
        step = 2 * (made - lent - 1) + pp * (layers + 2 * (lent - EARLY))
        still = functools.reduce(jnp.logical_or, [first & (made == m + 1) for m in LENDS], i == 0)

        for n in range(LENT):
            pl.when(first & (made == LENDS[n] + 1))(functools.partial(lend_out, n))

        @pl.when(jnp.logical_not(still))
        def _():
            pump(step)

        @pl.when(first)
        def _():
            @pl.when(i == 0)
            def _():
                down.wait_recv()
                c_cur[...] = z_in[...]

            c = c_cur[...]
            x1 = xb[2 + slot]

            def add(f, a, d):
                a1b[slot, :, cols(f)] += dot_tn(x1, d)
                a2b[slot, cols(f), :] += dot_tn(a.astype(BF16), c)

            c_cur[...] = chain(c, slot, slot, add)

        publish(made, slot)

        @pl.when(jnp.logical_not(still))
        def _():
            pump(step + 1)
        return carry

    lax.fori_loop(0, layers - EARLY * pp, grad_step, 0)

    @pl.when(first)
    def _():
        down.start()

    for i in (layers - 2, layers - 1):
        swap(i).wait_send()

    def tail_step(i, carry):
        pump(i)
        return carry

    ahead = pp * (layers - EARLY * SUB)
    lax.fori_loop(2 * (layers - LENT - 1) + pp * (layers + 2 * (LENT - EARLY)), chunks + ahead + 4 * LAG, tail_step, 0)

    @pl.when(first)
    def _():
        for n in range(LENT):
            lend(n).wait_send()
        for n in range(LENT * SUB):
            give_back(n).wait_recv()
            emit(LENDS[n // SUB] * SUB + n % SUB)

    @pl.when(pp == 1)
    def _():
        for n in range(LENT * SUB):
            give_back(n).wait_send()

    down.wait_send()

    @pl.when(pp == 1)
    def _():
        down.wait_recv()
        dx[...] = z_in[...]

    pltpu.make_async_copy(other, other, out_send).wait()
    pltpu.make_async_copy(other, other, out_recv).wait()


def widen(layers, blk, scale, own, other, dx, gi_hbm, go_hbm, dx_hbm, gi_buf, go_buf, gi_sem, go_sem, dx_sem):
    put_dx = pltpu.make_async_copy(dx, dx_hbm, dx_sem)
    put_dx.start()
    core = lax.rem(lax.axis_index('dp'), 2)
    pp = lax.axis_index('pp')
    rows = blk // SUB

    def step(i, carry):
        layer, slot = layer_of(pp, i, layers), lax.rem(i, 2)
        puts = (pltpu.make_async_copy(gi_buf.at[slot], gi_hbm.at[layer], gi_sem.at[slot]),
                pltpu.make_async_copy(go_buf.at[slot], go_hbm.at[layer], go_sem.at[slot]))

        @pl.when(i >= 2)
        def _():
            for put in puts:
                put.wait()

        def fill(gi, go):
            for q in range(4):
                for s in range(SUB):
                    r = slice(s * rows, (s + 1) * rows)
                    gi_buf[slot, r, q * blk:(q + 1) * blk] = gi[i * SUB + s, q].astype(F32) * scale
                    go_buf[slot, q * blk + s * rows:q * blk + (s + 1) * rows, :] = go[i * SUB + s, q].astype(F32) * scale

        pl.when(core == 0)(lambda: fill(own, other))
        pl.when(core == 1)(lambda: fill(other, own))
        for put in puts:
            put.start()
        return carry

    lax.fori_loop(0, layers, step, 0)
    for slot in range(2):
        pltpu.make_async_copy(gi_buf.at[slot], gi_hbm.at[slot], gi_sem.at[slot]).wait()
        pltpu.make_async_copy(go_buf.at[slot], go_hbm.at[slot], go_sem.at[slot]).wait()
    put_dx.wait()


def solution(mesh):
    replicas = mesh.shape['dp']

    def device_fn(w_in, w_out, x_saved, h_saved, dy_in, acc_in, acc_out):
        layers, hidden, ff = w_in.shape[1:]
        tokens = dy_in.shape[1]
        blk = ff // 4
        chunks, rows = layers * SUB, blk // SUB
        room = chunks + LENT * SUB
        dma = pltpu.SemaphoreType.DMA
        flops = 2 * tokens * hidden * ff * layers * 8
        call = pl.pallas_call(
            functools.partial(kernel, layers, blk),
            out_shape=(
                pltpu.VMEM((room, 4, rows, hidden), BF16),
                pltpu.VMEM((chunks, 4, rows, hidden), BF16),
                pltpu.VMEM((tokens, hidden), BF16),
                jax.ShapeDtypeStruct((layers, tokens, ff), BF16),
            ),
            in_specs=[pl.BlockSpec(memory_space=pl.ANY)] * 7,
            out_specs=[pl.BlockSpec(memory_space=pltpu.VMEM)] * 3 + [pl.BlockSpec(memory_space=pl.ANY)],
            scratch_shapes=[
                pltpu.VMEM((room, 4, rows, hidden), BF16),
                pltpu.VMEM((DEPTH, SUB, 4, rows, hidden), BF16),
                pltpu.VMEM((room, 2, rows, hidden), BF16),
                pltpu.VMEM((room, rows, hidden), BF16),
                pltpu.VMEM((2, SUB, 4, rows, hidden), BF16),
                pltpu.VMEM((2, hidden, ff), BF16),
                pltpu.VMEM((2, ff, hidden), BF16),
                pltpu.VMEM((4, tokens, ff), BF16),
                pltpu.VMEM((4, tokens, hidden), BF16),
                pltpu.VMEM((4, tokens, ff), BF16),
                pltpu.VMEM((2, hidden, ff), F32),
                pltpu.VMEM((2, ff, hidden), F32),
                pltpu.VMEM((layers, tokens, hidden), BF16),
                pltpu.VMEM((tokens, hidden), BF16),
                pltpu.VMEM((tokens, hidden), BF16),
                dma((2,)), dma((2,)), dma((4,)), dma((4,)), dma((2,)), dma((2,)), dma((2,)), dma((2,)), dma,
                dma((2,)), dma((DEPTH,)),
                dma((RING,)), dma((RING,)), dma((RING,)), dma((RING,)),
                dma((RING,)), dma((RING,)), dma((RING,)), dma((RING,)),
                dma, dma, dma, dma,
                dma((LENT,)), dma((LENT,)), dma((LENT * SUB,)), dma((LENT * SUB,)), pltpu.SemaphoreType.REGULAR,
            ],
            compiler_params=pltpu.CompilerParams(collective_id=0, has_side_effects=True, vmem_limit_bytes=67043328 - (35 << 19)),
            cost_estimate=pl.CostEstimate(flops=flops, bytes_accessed=200 << 20, transcendentals=0),
        )
        own, other, dx, _ = call(w_in, w_out, x_saved, h_saved, dy_in, acc_in, acc_out)
        grad_in, grad_out, dx_out = pl.pallas_call(
            functools.partial(widen, layers, blk, 1.0 / replicas),
            out_shape=(jax.ShapeDtypeStruct((layers, hidden, ff), F32), jax.ShapeDtypeStruct((layers, ff, hidden), F32),
                       jax.ShapeDtypeStruct((tokens, hidden), BF16)),
            in_specs=[pl.BlockSpec(memory_space=pltpu.VMEM)] * 3,
            out_specs=[pl.BlockSpec(memory_space=pl.ANY)] * 3,
            scratch_shapes=[pltpu.VMEM((2, hidden, ff), F32), pltpu.VMEM((2, ff, hidden), F32), dma((2,)), dma((2,)), dma],
            compiler_params=pltpu.CompilerParams(vmem_limit_bytes=12 << 20),
        )(own, other, dx)
        return grad_in[None], grad_out[None], dx_out[None]

    return jax.shard_map(device_fn, mesh=mesh, in_specs=(P('pp'), P('pp'), P('pp', None, None, 'dp'), P('pp', None, None, 'dp'), P('pp', 'dp'), P('pp', 'dp'), P('pp', 'dp')), out_specs=(P('pp'), P('pp'), P('pp', 'dp')), check_vma=False)
```

```python
import functools
import jax
import jax.numpy as jnp
from jax import lax
from jax.experimental import pallas as pl
from jax.experimental.pallas import tpu as pltpu
from jax.sharding import PartitionSpec as P

SUB = 2
LAG = 3
RING = 8
WIDEN_SLOTS = 4
DEPTH = 4
EARLY = 4
GAP = 4
SECOND = 3
LENDS = {4: (1,), 6: (1,), 8: (1,), 10: (1,)}
LENT = tuple(m * SUB + t for m, subs in LENDS.items() for t in subs)
TAKE_AT = 24
MESH = pl.DeviceIdType.MESH
ROOT_2_PI = 0.7978845608028654
CUBIC = 0.044715
F32 = jnp.float32
BF16 = jnp.bfloat16


def gelu_value(h):
    p = ROOT_2_PI + (ROOT_2_PI * CUBIC) * (h * h)
    s = 0.5 + 0.5 * jnp.tanh(h * p)
    return h * s


def gelu_slope(h):
    h2 = h * h
    p = ROOT_2_PI + (ROOT_2_PI * CUBIC) * h2
    s = 0.5 + 0.5 * jnp.tanh(h * p)
    a = h * s
    q = 2.0 * ROOT_2_PI + (6.0 * ROOT_2_PI * CUBIC) * h2
    return a, s + (a - a * s) * q


def dot_nt(a, b):
    return lax.dot_general(a, b, (((1,), (1,)), ((), ())), preferred_element_type=F32)


def dot_tn(a, b):
    return lax.dot_general(a, b, (((0,), (0,)), ((), ())), preferred_element_type=F32)


def layer_of(pp, made, layers):
    j = made - EARLY
    late = jnp.minimum(j + 1 + lax.div(j, GAP - 1), layers - 1)
    early = (made < EARLY).astype(jnp.int32)
    return layers - 1 - (made + pp * (late + early * (GAP * made - late) - made))


def kernel(layers, blk, w1_hbm, w2_hbm, x_hbm, h_hbm, dy_hbm, acc1_hbm, acc2_hbm,
           full, other, dx, dh_hbm,
           part, from_sib, rs1_in, rs2_in, to_sib,
           w1b, w2b, hb, xb, dhb, a1b, a2b, c_save, c_cur, z_in,
           sw1, sw2, sh, sx, sdh_in, sdh_out, sa1, sa2, s_misc,
           sib_send, sib_recv, rs1_send, rs1_recv, rs2_send, rs2_recv,
           ag2_send, ag2_recv, ag1_send, ag1_recv, out_send, out_recv,
           z_send, z_recv,
           lend_send, lend_recv, back_send, back_recv, sib_free):
    pp = lax.axis_index('pp')
    dp = lax.axis_index('dp')
    core = lax.rem(dp, 2)
    bx = lax.rem(lax.div(dp, 2), 2)
    by = lax.div(dp, 4)
    b1 = bx + core * (by - bx)
    b2 = by + core * (bx - by)
    d1 = 2 + 2 * core
    d2 = 4 - 2 * core
    n1 = dp + (1 - 2 * b1) * d1
    n2 = dp + (1 - 2 * b2) * d2
    sib = dp + 1 - 2 * core
    quarter = 2 * b1 + b2
    first = pp == 0
    chunks = layers * SUB - len(LENT) + 2 * len(LENT) * pp
    rows = blk // SUB

    def load_w(layer, slot):
        return (pltpu.make_async_copy(w1_hbm.at[0, layer], w1b.at[slot], sw1.at[slot]),
                pltpu.make_async_copy(w2_hbm.at[0, layer], w2b.at[slot], sw2.at[slot]))

    def load_h(micro, layer, slot):
        return pltpu.make_async_copy(h_hbm.at[0, micro, layer], hb.at[slot], sh.at[slot])

    def load_x(micro, layer, slot):
        return pltpu.make_async_copy(x_hbm.at[0, micro, layer], xb.at[slot], sx.at[slot])

    def load_sums(layer, slot):
        return (pltpu.make_async_copy(acc1_hbm.at[0, 0, layer], a1b.at[slot], sa1.at[slot]),
                pltpu.make_async_copy(acc2_hbm.at[0, 0, layer], a2b.at[slot], sa2.at[slot]),
                load_x(0, layer, slot))

    def load_rest(layer, slot):
        return load_sums(layer, slot) + (
            pltpu.make_async_copy(dh_hbm.at[layer], dhb.at[2 + slot], sdh_in.at[slot]),
            load_h(0, layer, 2 + slot))

    def load_second(layer, slot):
        return load_w(layer, slot) + (load_h(1, layer, slot), load_x(1, layer, 2 + slot))

    def save_dh(layer, slot):
        return pltpu.make_async_copy(dhb.at[slot], dh_hbm.at[layer], sdh_out.at[slot])

    def start_grad(step):
        layer, slot = layer_of(pp, step + EARLY * pp, layers), lax.rem(step, 2)
        for copy in load_rest(layer, slot):
            copy.start()

        @pl.when(first)
        def _():
            for copy in load_second(layer, slot):
                copy.start()

    def place(k):
        late = sum((k >= c - n).astype(jnp.int32) for n, c in enumerate(LENT))
        after = (k >= TAKE_AT).astype(jnp.int32)
        past = (k >= TAKE_AT + len(LENT)).astype(jnp.int32)
        one = k + (layers * SUB - TAKE_AT) * (after - past) - len(LENT) * past
        return k + late + pp * (one - k - late)

    def remote(src, dst, send, recv, peer):
        return pltpu.make_async_remote_copy(src, dst, send, recv, device_id=peer, device_id_type=MESH)

    def rs1(k):
        b, r = place(k), lax.rem(k, RING)
        return remote(part.at[b, pl.ds(2 * (1 - b1), 2)], rs1_in.at[b], rs1_send.at[r], rs1_recv.at[r], (pp, n1))

    def rs2(k):
        b, r = place(k), lax.rem(k, RING)
        return remote(part.at[b, 2 * b1 + 1 - b2], rs2_in.at[b], rs2_send.at[r], rs2_recv.at[r], (pp, n2))

    def ag2(k):
        b, r = place(k), lax.rem(k, RING)
        return remote(full.at[b, quarter], full.at[b, quarter], ag2_send.at[r], ag2_recv.at[r], (pp, n2))

    def ag1(k):
        b, r = place(k), lax.rem(k, RING)
        mine = full.at[b, pl.ds(2 * b1, 2)]
        return remote(mine, mine, ag1_send.at[r], ag1_recv.at[r], (pp, n1))

    def swap(made):
        slot, held = lax.rem(made, 2), lax.rem(made, DEPTH)
        return remote(to_sib.at[slot], from_sib.at[held], sib_send.at[slot], sib_recv.at[held], (pp, sib))

    def freed(made):
        @pl.when(made + DEPTH < layers)
        def _():
            pl.semaphore_signal(sib_free, inc=1, device_id=(pp, sib), device_id_type=MESH)

    def lend(n):
        return remote(part.at[LENT[n]], part.at[layers * SUB + n], lend_send.at[n], lend_recv.at[n], (1 - pp, dp))

    def give_back(n):
        return remote(full.at[layers * SUB + n], full.at[LENT[n]], back_send.at[n], back_recv.at[n], (1 - pp, dp))

    def emit(b):
        remote(full.at[b], other.at[b], out_send, out_recv, (pp, sib)).start()

    def lend_out(made):
        if 0 in LENDS[made]:
            swap(made).wait_recv()
        for t in LENDS[made]:
            c = made * SUB + t
            part[c] = part[c] + from_sib[made % DEPTH, t]
        freed(made)
        for t in LENDS[made]:
            lend(LENT.index(made * SUB + t)).start()

    def chunk_at(step):
        turn, at = lax.div(step, GAP), lax.rem(step, GAP)
        chain = (step < layers + SUB).astype(jnp.int32)
        one = (1 - chain) * (step - layers - SUB + EARLY * SUB) + chain * (2 * turn + (at == SECOND).astype(jnp.int32))
        k = step + pp * (one - step)
        idle = (pp == 1) & (chain == 1) & ((turn >= EARLY) | ((at != 1) & (at != SECOND)))
        return k, (step >= 0) & (k < chunks) & jnp.logical_not(idle)

    def pump(i):
        def phase(n, body):
            k, there = chunk_at(i - n * LAG)
            pl.when(there)(lambda: body(k))

        def sum0(k):
            b = place(k)
            made, sub = lax.div(b, SUB), lax.rem(b, SUB)

            @pl.when(made < layers)
            def _():
                @pl.when(sub == 0)
                def _():
                    swap(made).wait_recv()
                part[b] = part[b] + from_sib[lax.rem(made, DEPTH), sub]

                @pl.when(sub == SUB - 1)
                def _():
                    freed(made)

            for n in range(len(LENT)):
                pl.when(b == layers * SUB + n)(lambda n=n: lend(n).wait_recv())

        def sum1(k):
            rs1(k).wait()
            b = place(k)
            for j in range(2):
                part[b, 2 * b1 + j] = part[b, 2 * b1 + j] + rs1_in[b, j]

        def sum2(k):
            rs2(k).wait()
            b = place(k)
            full[b, quarter] = part[b, quarter] + rs2_in[b]

        def done2(k):
            ag2(k).wait()
            ag1(k).start()

        def done1(k):
            ag1(k).wait()
            b = place(k)
            pl.when(b < layers * SUB)(lambda: emit(b))
            for n in range(len(LENT)):
                pl.when(b == layers * SUB + n)(lambda n=n: give_back(n).start())

        phase(2, sum2)
        phase(1, sum1)
        phase(0, sum0)
        phase(3, done2)
        phase(2, lambda k: ag2(k).start())
        phase(1, lambda k: rs2(k).start())
        phase(0, lambda k: rs1(k).start())
        phase(4, done1)

    def cols(f):
        return slice(f * blk, (f + 1) * blk)

    first_c = pltpu.make_async_copy(dy_hbm.at[0], c_cur, s_misc)
    first_c.start()
    for copy in load_w(layers - 1, 0) + (load_h(0, layers - 1, 0),):
        copy.start()
    @pl.when(pp == 1)
    def _():
        for copy in load_sums(layers - 1, 0):
            copy.start()

    barrier = pltpu.get_barrier_semaphore()
    for peer in ((pp, sib), (pp, n1), (pp, n2), (1 - pp, dp)):
        pl.semaphore_signal(barrier, inc=1, device_id=peer, device_id_type=MESH)
    pl.semaphore_wait(barrier, 4)
    first_c.wait()

    def chain(c, hs, ws, with_grads):
        total = None
        for f in range(4):
            h = hb[hs, :, cols(f)].astype(F32)
            a, slope = gelu_slope(h)
            d = (dot_nt(c, w2b[ws, cols(f), :]) * slope).astype(BF16)
            with_grads(f, a, d)
            back = dot_nt(d, w1b[ws, :, cols(f)])
            total = back if total is None else total + back
        return (c.astype(F32) + total).astype(BF16)

    def first_grads(layer, slot, hs, ds):
        x0 = xb[slot]
        c0 = c_save[layer]
        for f in range(4):
            a = gelu_value(hb[hs, :, cols(f)].astype(F32)).astype(BF16)
            a1b[slot, :, cols(f)] += dot_tn(x0, dhb[ds, :, cols(f)])
            a2b[slot, cols(f), :] += dot_tn(a, c0)

    def publish(made, slot):
        @pl.when(made >= 2)
        def _():
            swap(made - 2).wait_send()

        for f in range(4):
            g1 = a1b[slot, :, cols(f)].astype(BF16)
            g2 = a2b[slot, cols(f), :].astype(BF16)
            own = jnp.where(core == 0, g1, g2)
            rest = jnp.where(core == 0, g2, g1)
            for t in range(SUB):
                part[made * SUB + t, f] = own[t * rows:(t + 1) * rows]
                to_sib[lax.rem(made, 2), t, f] = rest[t * rows:(t + 1) * rows]

        @pl.when(made >= DEPTH)
        def _():
            pl.semaphore_wait(sib_free, 1)
        swap(made).start()

    def chain_step(i, carry):
        layer, slot = layers - 1 - i, lax.rem(i, 2)
        for copy in load_w(layer, slot) + (load_h(0, layer, slot),):
            copy.wait()

        @pl.when(i + 1 < layers)
        def _():
            for copy in load_w(layer - 1, 1 - slot) + (load_h(0, layer - 1, 1 - slot),):
                copy.start()

        @pl.when(i + 1 == layers)
        def _():
            start_grad(0)

        @pl.when(i >= 2)
        def _():
            save_dh(layer + 2, slot).wait()

        c = c_cur[...]
        c_save[layer] = c

        def keep(f, a, d):
            dhb[slot, :, cols(f)] = d

        c_cur[...] = chain(c, slot, slot, keep)
        save_dh(layer, slot).start()

        turn, at = lax.div(i, GAP), lax.rem(i, GAP)

        @pl.when((pp == 1) & (at == 0) & (turn < EARLY))
        def _():
            held = lax.rem(turn, 2)
            for copy in load_sums(layer, held):
                copy.wait()

            @pl.when(turn + 1 < EARLY)
            def _():
                for copy in load_sums(layer - GAP, 1 - held):
                    copy.start()

            first_grads(layer, held, slot, slot)
            publish(turn, held)

        @pl.when((pp == 1) & (i > 0))
        def _():
            pump(i)
        return carry

    lax.fori_loop(0, layers, chain_step, 0)

    down = pltpu.make_async_remote_copy(c_cur, z_in, z_send, z_recv, device_id=(1 - pp, dp), device_id_type=MESH)

    @pl.when(pp == 1)
    def _():
        down.start()

    @pl.when(first)
    def _():
        dx[...] = c_cur[...]

    save_dh(1, lax.rem(layers, 2)).wait()
    save_dh(0, lax.rem(layers + 1, 2)).wait()

    def grad_step(i, carry):
        made = i + EARLY * pp
        layer, slot = layer_of(pp, made, layers), lax.rem(i, 2)
        for copy in load_rest(layer, slot):
            copy.wait()

        @pl.when(first)
        def _():
            for copy in load_second(layer, slot):
                copy.wait()

        @pl.when(made + 1 < layers)
        def _():
            start_grad(i + 1)

        first_grads(layer, slot, 2 + slot, 2 + slot)

        def ready(m):
            return m * SUB - (1 - pp) * sum((m * SUB > c).astype(jnp.int32) for c in LENT)

        step = ready(made - 1) + pp * (layers + SUB - EARLY * SUB)
        count = jnp.where(made == 0, 0, ready(made) - ready(made - 1))

        @pl.when(count > 0)
        def _():
            pump(step)

        for m in LENDS:
            pl.when(first & (made == m + 1))(functools.partial(lend_out, m))

        @pl.when(first)
        def _():
            @pl.when(i == 0)
            def _():
                down.wait_recv()
                c_cur[...] = z_in[...]

            c = c_cur[...]
            x1 = xb[2 + slot]

            def add(f, a, d):
                a1b[slot, :, cols(f)] += dot_tn(x1, d)
                a2b[slot, cols(f), :] += dot_tn(a.astype(BF16), c)

            c_cur[...] = chain(c, slot, slot, add)

        publish(made, slot)

        @pl.when(count > 1)
        def _():
            pump(step + 1)
        return carry

    lax.fori_loop(0, layers - EARLY * pp, grad_step, 0)

    @pl.when(first)
    def _():
        down.start()

    for i in (layers - 2, layers - 1):
        swap(i).wait_send()

    def tail_step(i, carry):
        pump(i)
        return carry

    ahead = pp * (layers + SUB - EARLY * SUB)
    behind = (layers - 1) * SUB - (1 - pp) * sum(c < (layers - 1) * SUB for c in LENT)
    lax.fori_loop(behind + ahead, chunks + ahead + 4 * LAG, tail_step, 0)

    @pl.when(first)
    def _():
        for n in range(len(LENT)):
            lend(n).wait_send()
            give_back(n).wait_recv()
            emit(LENT[n])

    @pl.when(pp == 1)
    def _():
        for n in range(len(LENT)):
            give_back(n).wait_send()

    down.wait_send()

    @pl.when(pp == 1)
    def _():
        down.wait_recv()
        dx[...] = z_in[...]

    pltpu.make_async_copy(other, other, out_send).wait()
    pltpu.make_async_copy(other, other, out_recv).wait()


def widen(layers, blk, scale, own, other, dx, gi_hbm, go_hbm, dx_hbm, gi_buf, go_buf, gi_sem, go_sem, dx_sem):
    put_dx = pltpu.make_async_copy(dx, dx_hbm, dx_sem)
    put_dx.start()
    core = lax.rem(lax.axis_index('dp'), 2)
    pp = lax.axis_index('pp')
    rows = blk // SUB

    def step(i, carry):
        layer, slot = layer_of(pp, i, layers), lax.rem(i, WIDEN_SLOTS)
        puts = (pltpu.make_async_copy(gi_buf.at[slot], gi_hbm.at[layer], gi_sem.at[slot]),
                pltpu.make_async_copy(go_buf.at[slot], go_hbm.at[layer], go_sem.at[slot]))

        @pl.when(i >= WIDEN_SLOTS)
        def _():
            for put in puts:
                put.wait()

        def fill(gi, go):
            for q in range(4):
                for s in range(SUB):
                    r = slice(s * rows, (s + 1) * rows)
                    gi_buf[slot, r, q * blk:(q + 1) * blk] = gi[i * SUB + s, q].astype(F32) * scale
                    go_buf[slot, q * blk + s * rows:q * blk + (s + 1) * rows, :] = go[i * SUB + s, q].astype(F32) * scale

        pl.when(core == 0)(lambda: fill(own, other))
        pl.when(core == 1)(lambda: fill(other, own))
        for put in puts:
            put.start()
        return carry

    lax.fori_loop(0, layers, step, 0)
    for slot in range(WIDEN_SLOTS):
        pltpu.make_async_copy(gi_buf.at[slot], gi_hbm.at[slot], gi_sem.at[slot]).wait()
        pltpu.make_async_copy(go_buf.at[slot], go_hbm.at[slot], go_sem.at[slot]).wait()
    put_dx.wait()


def solution(mesh):
    replicas = mesh.shape['dp']

    def device_fn(w_in, w_out, x_saved, h_saved, dy_in, acc_in, acc_out):
        layers, hidden, ff = w_in.shape[1:]
        tokens = dy_in.shape[1]
        blk = ff // 4
        chunks, rows = layers * SUB, blk // SUB
        room = chunks + len(LENT)
        dma = pltpu.SemaphoreType.DMA
        flops = 2 * tokens * hidden * ff * layers * 8
        call = pl.pallas_call(
            functools.partial(kernel, layers, blk),
            out_shape=(
                pltpu.VMEM((room, 4, rows, hidden), BF16),
                pltpu.VMEM((chunks, 4, rows, hidden), BF16),
                pltpu.VMEM((tokens, hidden), BF16),
                jax.ShapeDtypeStruct((layers, tokens, ff), BF16),
            ),
            in_specs=[pl.BlockSpec(memory_space=pl.ANY)] * 7,
            out_specs=[pl.BlockSpec(memory_space=pltpu.VMEM)] * 3 + [pl.BlockSpec(memory_space=pl.ANY)],
            scratch_shapes=[
                pltpu.VMEM((room, 4, rows, hidden), BF16),
                pltpu.VMEM((DEPTH, SUB, 4, rows, hidden), BF16),
                pltpu.VMEM((room, 2, rows, hidden), BF16),
                pltpu.VMEM((room, rows, hidden), BF16),
                pltpu.VMEM((2, SUB, 4, rows, hidden), BF16),
                pltpu.VMEM((2, hidden, ff), BF16),
                pltpu.VMEM((2, ff, hidden), BF16),
                pltpu.VMEM((4, tokens, ff), BF16),
                pltpu.VMEM((4, tokens, hidden), BF16),
                pltpu.VMEM((4, tokens, ff), BF16),
                pltpu.VMEM((2, hidden, ff), F32),
                pltpu.VMEM((2, ff, hidden), F32),
                pltpu.VMEM((layers, tokens, hidden), BF16),
                pltpu.VMEM((tokens, hidden), BF16),
                pltpu.VMEM((tokens, hidden), BF16),
                dma((2,)), dma((2,)), dma((4,)), dma((4,)), dma((2,)), dma((2,)), dma((2,)), dma((2,)), dma,
                dma((2,)), dma((DEPTH,)),
                dma((RING,)), dma((RING,)), dma((RING,)), dma((RING,)),
                dma((RING,)), dma((RING,)), dma((RING,)), dma((RING,)),
                dma, dma, dma, dma,
                dma((len(LENT),)), dma((len(LENT),)), dma((len(LENT),)), dma((len(LENT),)), pltpu.SemaphoreType.REGULAR,
            ],
            compiler_params=pltpu.CompilerParams(collective_id=0, has_side_effects=True, vmem_limit_bytes=67043328 - (36 << 19)),
            cost_estimate=pl.CostEstimate(flops=flops, bytes_accessed=200 << 20, transcendentals=0),
        )
        own, other, dx, _ = call(w_in, w_out, x_saved, h_saved, dy_in, acc_in, acc_out)
        grad_in, grad_out, dx_out = pl.pallas_call(
            functools.partial(widen, layers, blk, 1.0 / replicas),
            out_shape=(jax.ShapeDtypeStruct((layers, hidden, ff), F32), jax.ShapeDtypeStruct((layers, ff, hidden), F32),
                       jax.ShapeDtypeStruct((tokens, hidden), BF16)),
            in_specs=[pl.BlockSpec(memory_space=pltpu.VMEM)] * 3,
            out_specs=[pl.BlockSpec(memory_space=pl.ANY)] * 3,
            scratch_shapes=[pltpu.VMEM((WIDEN_SLOTS, hidden, ff), F32), pltpu.VMEM((WIDEN_SLOTS, ff, hidden), F32),
                            dma((WIDEN_SLOTS,)), dma((WIDEN_SLOTS,)), dma],
            compiler_params=pltpu.CompilerParams(vmem_limit_bytes=24 << 20),
        )(own, other, dx)
        return grad_in[None], grad_out[None], dx_out[None]

    return jax.shard_map(device_fn, mesh=mesh, in_specs=(P('pp'), P('pp'), P('pp', None, None, 'dp'), P('pp', None, None, 'dp'), P('pp', 'dp'), P('pp', 'dp'), P('pp', 'dp')), out_specs=(P('pp'), P('pp'), P('pp', 'dp')), check_vma=False)
```

```python
import functools
import jax
import jax.numpy as jnp
from jax import lax
from jax.experimental import pallas as pl
from jax.experimental.pallas import tpu as pltpu
from jax.sharding import PartitionSpec as P

SUB = 2
LAG = 3
RING = 8
WIDEN_SLOTS = 4
DEPTH = 4
EARLY = 4
GAP = 4
SECOND = 3
LENDS = {4: (1,), 5: (1,), 6: (1,), 7: (1,)}
LENT = tuple(m * SUB + t for m, subs in LENDS.items() for t in subs)
TAKE_AT = 22
MESH = pl.DeviceIdType.MESH
ROOT_2_PI = 0.7978845608028654
CUBIC = 0.044715
F32 = jnp.float32
BF16 = jnp.bfloat16


def gelu_value(h):
    p = ROOT_2_PI + (ROOT_2_PI * CUBIC) * (h * h)
    s = 0.5 + 0.5 * jnp.tanh(h * p)
    return h * s


def gelu_slope(h):
    h2 = h * h
    p = ROOT_2_PI + (ROOT_2_PI * CUBIC) * h2
    s = 0.5 + 0.5 * jnp.tanh(h * p)
    a = h * s
    q = 2.0 * ROOT_2_PI + (6.0 * ROOT_2_PI * CUBIC) * h2
    return a, s + (a - a * s) * q


def twice_slope(h):
    h2 = h * h
    t = jnp.tanh(h * (ROOT_2_PI + (ROOT_2_PI * CUBIC) * h2))
    q = ROOT_2_PI + (3.0 * ROOT_2_PI * CUBIC) * h2
    return None, (t + ((1.0 - t * t) * h) * q) + 1.0


def dot_nt(a, b):
    return lax.dot_general(a, b, (((1,), (1,)), ((), ())), preferred_element_type=F32)


def dot_tn(a, b):
    return lax.dot_general(a, b, (((0,), (0,)), ((), ())), preferred_element_type=F32)


def layer_of(pp, made, layers):
    j = made - EARLY
    late = jnp.minimum(j + 1 + lax.div(j, GAP - 1), layers - 1)
    early = (made < EARLY).astype(jnp.int32)
    return layers - 1 - (made + pp * (late + early * (GAP * made - late) - made))


def kernel(layers, blk, w1_hbm, w2_hbm, x_hbm, h_hbm, dy_hbm, acc1_hbm, acc2_hbm,
           full, other, dx, dh_hbm,
           part, from_sib, rs1_in, rs2_in, to_sib,
           w1b, w2b, hb, xb, dhb, a1b, a2b, c_save, c_cur, z_in,
           sw1, sw2, sh, sx, sdh_in, sdh_out, sa1, sa2, s_misc,
           sib_send, sib_recv, rs1_send, rs1_recv, rs2_send, rs2_recv,
           ag2_send, ag2_recv, ag1_send, ag1_recv, out_send, out_recv,
           z_send, z_recv,
           lend_send, lend_recv, back_send, back_recv, sib_free):
    pp = lax.axis_index('pp')
    dp = lax.axis_index('dp')
    core = lax.rem(dp, 2)
    bx = lax.rem(lax.div(dp, 2), 2)
    by = lax.div(dp, 4)
    b1 = bx + core * (by - bx)
    b2 = by + core * (bx - by)
    d1 = 2 + 2 * core
    d2 = 4 - 2 * core
    n1 = dp + (1 - 2 * b1) * d1
    n2 = dp + (1 - 2 * b2) * d2
    sib = dp + 1 - 2 * core
    quarter = 2 * b1 + b2
    first = pp == 0
    chunks = layers * SUB - len(LENT) + 2 * len(LENT) * pp
    rows = blk // SUB

    def load_w(layer, slot):
        return (pltpu.make_async_copy(w1_hbm.at[0, layer], w1b.at[slot], sw1.at[slot]),
                pltpu.make_async_copy(w2_hbm.at[0, layer], w2b.at[slot], sw2.at[slot]))

    def load_h(micro, layer, slot):
        return pltpu.make_async_copy(h_hbm.at[0, micro, layer], hb.at[slot], sh.at[slot])

    def load_x(micro, layer, slot):
        return pltpu.make_async_copy(x_hbm.at[0, micro, layer], xb.at[slot], sx.at[slot])

    def load_sums(layer, slot):
        return (pltpu.make_async_copy(acc1_hbm.at[0, 0, layer], a1b.at[slot], sa1.at[slot]),
                pltpu.make_async_copy(acc2_hbm.at[0, 0, layer], a2b.at[slot], sa2.at[slot]),
                load_x(0, layer, slot))

    def load_rest(layer, slot):
        return load_sums(layer, slot) + (
            pltpu.make_async_copy(dh_hbm.at[layer], dhb.at[2 + slot], sdh_in.at[slot]),
            load_h(0, layer, 2 + slot))

    def load_second(layer, slot):
        return load_w(layer, slot) + (load_h(1, layer, slot), load_x(1, layer, 2 + slot))

    def save_dh(layer, slot):
        return pltpu.make_async_copy(dhb.at[slot], dh_hbm.at[layer], sdh_out.at[slot])

    def start_grad(step):
        layer, slot = layer_of(pp, step + EARLY * pp, layers), lax.rem(step, 2)
        for copy in load_rest(layer, slot):
            copy.start()

        @pl.when(first)
        def _():
            for copy in load_second(layer, slot):
                copy.start()

    def place(k):
        late = sum((k >= c - n).astype(jnp.int32) for n, c in enumerate(LENT))
        after = (k >= TAKE_AT).astype(jnp.int32)
        past = (k >= TAKE_AT + len(LENT)).astype(jnp.int32)
        one = k + (layers * SUB - TAKE_AT) * (after - past) - len(LENT) * past
        return k + late + pp * (one - k - late)

    def remote(src, dst, send, recv, peer):
        return pltpu.make_async_remote_copy(src, dst, send, recv, device_id=peer, device_id_type=MESH)

    def rs1(k):
        b, r = place(k), lax.rem(k, RING)
        return remote(part.at[b, pl.ds(2 * (1 - b1), 2)], rs1_in.at[b], rs1_send.at[r], rs1_recv.at[r], (pp, n1))

    def rs2(k):
        b, r = place(k), lax.rem(k, RING)
        return remote(part.at[b, 2 * b1 + 1 - b2], rs2_in.at[b], rs2_send.at[r], rs2_recv.at[r], (pp, n2))

    def ag2(k):
        b, r = place(k), lax.rem(k, RING)
        return remote(full.at[b, quarter], full.at[b, quarter], ag2_send.at[r], ag2_recv.at[r], (pp, n2))

    def ag1(k):
        b, r = place(k), lax.rem(k, RING)
        mine = full.at[b, pl.ds(2 * b1, 2)]
        return remote(mine, mine, ag1_send.at[r], ag1_recv.at[r], (pp, n1))

    def swap(made):
        slot, held = lax.rem(made, 2), lax.rem(made, DEPTH)
        return remote(to_sib.at[slot], from_sib.at[held], sib_send.at[slot], sib_recv.at[held], (pp, sib))

    def freed(made):
        @pl.when(made + DEPTH < layers)
        def _():
            pl.semaphore_signal(sib_free, inc=1, device_id=(pp, sib), device_id_type=MESH)

    def lend(n):
        return remote(part.at[LENT[n]], part.at[layers * SUB + n], lend_send.at[n], lend_recv.at[n], (1 - pp, dp))

    def give_back(n):
        return remote(full.at[layers * SUB + n], full.at[LENT[n]], back_send.at[n], back_recv.at[n], (1 - pp, dp))

    def emit(b):
        remote(full.at[b], other.at[b], out_send, out_recv, (pp, sib)).start()

    def lend_out(made):
        if 0 in LENDS[made]:
            swap(made).wait_recv()
        for t in LENDS[made]:
            c = made * SUB + t
            part[c] = part[c] + from_sib[made % DEPTH, t]
        freed(made)
        for t in LENDS[made]:
            lend(LENT.index(made * SUB + t)).start()

    def chunk_at(step):
        turn, at = lax.div(step, GAP), lax.rem(step, GAP)
        chain = (step < layers + SUB).astype(jnp.int32)
        one = (1 - chain) * (step - layers - SUB + EARLY * SUB) + chain * (2 * turn + (at == SECOND).astype(jnp.int32))
        k = step + pp * (one - step)
        idle = (pp == 1) & (chain == 1) & ((turn >= EARLY) | ((at != 1) & (at != SECOND)))
        return k, (step >= 0) & (k < chunks) & jnp.logical_not(idle)

    def pump(i):
        def phase(n, body):
            k, there = chunk_at(i - n * LAG)
            pl.when(there)(lambda: body(k))

        def sum0(k):
            b = place(k)
            made, sub = lax.div(b, SUB), lax.rem(b, SUB)

            @pl.when(made < layers)
            def _():
                @pl.when(sub == 0)
                def _():
                    swap(made).wait_recv()
                part[b] = part[b] + from_sib[lax.rem(made, DEPTH), sub]

                @pl.when(sub == SUB - 1)
                def _():
                    freed(made)

            for n in range(len(LENT)):
                pl.when(b == layers * SUB + n)(lambda n=n: lend(n).wait_recv())

        def sum1(k):
            rs1(k).wait()
            b = place(k)
            for j in range(2):
                part[b, 2 * b1 + j] = part[b, 2 * b1 + j] + rs1_in[b, j]

        def sum2(k):
            rs2(k).wait()
            b = place(k)
            full[b, quarter] = part[b, quarter] + rs2_in[b]

        def done2(k):
            ag2(k).wait()
            ag1(k).start()

        def done1(k):
            ag1(k).wait()
            b = place(k)
            pl.when(b < layers * SUB)(lambda: emit(b))
            for n in range(len(LENT)):
                pl.when(b == layers * SUB + n)(lambda n=n: give_back(n).start())

        phase(2, sum2)
        phase(1, sum1)
        phase(0, sum0)
        phase(3, done2)
        phase(2, lambda k: ag2(k).start())
        phase(1, lambda k: rs2(k).start())
        phase(0, lambda k: rs1(k).start())
        phase(4, done1)

    def cols(f):
        return slice(f * blk, (f + 1) * blk)

    first_c = pltpu.make_async_copy(dy_hbm.at[0], c_cur, s_misc)
    first_c.start()
    for copy in load_w(layers - 1, 0) + (load_h(0, layers - 1, 0),):
        copy.start()
    @pl.when(pp == 1)
    def _():
        for copy in load_sums(layers - 1, 0):
            copy.start()

    barrier = pltpu.get_barrier_semaphore()
    for peer in ((pp, sib), (pp, n1), (pp, n2), (1 - pp, dp)):
        pl.semaphore_signal(barrier, inc=1, device_id=peer, device_id_type=MESH)
    pl.semaphore_wait(barrier, 4)
    first_c.wait()

    def chain(c, hs, ws, with_grads, slope_of=gelu_slope, scale=1.0):
        total = None
        c_in = (c * jnp.asarray(scale, c.dtype))
        for f in range(4):
            h = hb[hs, :, cols(f)].astype(F32)
            a, slope = slope_of(h)
            d = (dot_nt(c_in, w2b[ws, cols(f), :]) * slope).astype(BF16)
            with_grads(f, a, d)
            back = dot_nt(d, w1b[ws, :, cols(f)])
            total = back if total is None else total + back
        return (c.astype(F32) + total).astype(BF16)

    def first_grads(layer, slot, hs, ds):
        x0 = xb[slot]
        c0 = c_save[layer]
        for f in range(4):
            a = gelu_value(hb[hs, :, cols(f)].astype(F32)).astype(BF16)
            a1b[slot, :, cols(f)] += dot_tn(x0, dhb[ds, :, cols(f)])
            a2b[slot, cols(f), :] += dot_tn(a, c0)

    def publish(made, slot):
        @pl.when(made >= 2)
        def _():
            swap(made - 2).wait_send()

        for f in range(4):
            g1 = a1b[slot, :, cols(f)].astype(BF16)
            g2 = a2b[slot, cols(f), :].astype(BF16)
            own = jnp.where(core == 0, g1, g2)
            rest = jnp.where(core == 0, g2, g1)
            for t in range(SUB):
                part[made * SUB + t, f] = own[t * rows:(t + 1) * rows]
                to_sib[lax.rem(made, 2), t, f] = rest[t * rows:(t + 1) * rows]

        @pl.when(made >= DEPTH)
        def _():
            pl.semaphore_wait(sib_free, 1)
        swap(made).start()

    def down():
        return remote(c_cur, z_in, z_send, z_recv, (1 - pp, dp))

    def chain_step(i, carry):
        layer, slot = layers - 1 - i, lax.rem(i, 2)
        for copy in load_w(layer, slot) + (load_h(0, layer, slot),):
            copy.wait()

        @pl.when(i + 1 < layers)
        def _():
            for copy in load_w(layer - 1, 1 - slot) + (load_h(0, layer - 1, 1 - slot),):
                copy.start()

        @pl.when(i + 1 == layers)
        def _():
            start_grad(0)

        @pl.when(i >= 2)
        def _():
            save_dh(layer + 2, slot).wait()

        c = c_cur[...]
        c_save[layer] = c

        def keep(f, a, d):
            dhb[slot, :, cols(f)] = d

        c_cur[...] = chain(c, slot, slot, keep, twice_slope, 0.5)
        save_dh(layer, slot).start()

        @pl.when((pp == 1) & (i + 1 == layers))
        def _():
            down().start()

        turn, at = lax.div(i, GAP), lax.rem(i, GAP)

        @pl.when((pp == 1) & (at == 0) & (turn < EARLY))
        def _():
            held = lax.rem(turn, 2)
            for copy in load_sums(layer, held):
                copy.wait()

            @pl.when(turn + 1 < EARLY)
            def _():
                for copy in load_sums(layer - GAP, 1 - held):
                    copy.start()

            first_grads(layer, held, slot, slot)
            publish(turn, held)

        @pl.when((pp == 1) & (i > 0))
        def _():
            pump(i)
        return carry

    lax.fori_loop(0, layers, chain_step, 0)


    @pl.when(first)
    def _():
        dx[...] = c_cur[...]

    save_dh(1, lax.rem(layers, 2)).wait()
    save_dh(0, lax.rem(layers + 1, 2)).wait()

    def grad_step(i, carry):
        made = i + EARLY * pp
        layer, slot = layer_of(pp, made, layers), lax.rem(i, 2)
        for copy in load_rest(layer, slot):
            copy.wait()

        @pl.when(first)
        def _():
            for copy in load_second(layer, slot):
                copy.wait()

        @pl.when(made + 1 < layers)
        def _():
            start_grad(i + 1)

        first_grads(layer, slot, 2 + slot, 2 + slot)

        def ready(m):
            return m * SUB - (1 - pp) * sum((m * SUB > c).astype(jnp.int32) for c in LENT)

        step = ready(made - 1) + pp * (layers + SUB - EARLY * SUB)
        count = jnp.where(made == 0, 0, ready(made) - ready(made - 1))

        @pl.when(count > 0)
        def _():
            pump(step)

        for m in LENDS:
            pl.when(first & (made == m + 1))(functools.partial(lend_out, m))

        @pl.when(first)
        def _():
            @pl.when(i == 0)
            def _():
                down().wait_recv()
                c_cur[...] = z_in[...]

            c = c_cur[...]
            x1 = xb[2 + slot]

            def add(f, a, d):
                a1b[slot, :, cols(f)] += dot_tn(x1, d)
                a2b[slot, cols(f), :] += dot_tn(a.astype(BF16), c)

            c_cur[...] = chain(c, slot, slot, add)

        publish(made, slot)

        @pl.when(count > 1)
        def _():
            pump(step + 1)
        return carry

    lax.fori_loop(0, layers - EARLY * pp, grad_step, 0)

    @pl.when(first)
    def _():
        down().start()

    for i in (layers - 2, layers - 1):
        swap(i).wait_send()

    def tail_step(i, carry):
        pump(i)
        return carry

    ahead = pp * (layers + SUB - EARLY * SUB)
    behind = (layers - 1) * SUB - (1 - pp) * sum(c < (layers - 1) * SUB for c in LENT)
    lax.fori_loop(behind + ahead, chunks + ahead + 4 * LAG, tail_step, 0)

    @pl.when(first)
    def _():
        for n in range(len(LENT)):
            lend(n).wait_send()
            give_back(n).wait_recv()
            emit(LENT[n])

    @pl.when(pp == 1)
    def _():
        for n in range(len(LENT)):
            give_back(n).wait_send()

    down().wait_send()

    @pl.when(pp == 1)
    def _():
        down().wait_recv()
        dx[...] = z_in[...]

    pltpu.make_async_copy(other, other, out_send).wait()
    pltpu.make_async_copy(other, other, out_recv).wait()


def widen(layers, blk, scale, own, other, dx, gi_hbm, go_hbm, dx_hbm, gi_buf, go_buf, gi_sem, go_sem, dx_sem):
    put_dx = pltpu.make_async_copy(dx, dx_hbm, dx_sem)
    put_dx.start()
    core = lax.rem(lax.axis_index('dp'), 2)
    pp = lax.axis_index('pp')
    rows = blk // SUB

    def step(i, carry):
        layer, slot = layer_of(pp, i, layers), lax.rem(i, WIDEN_SLOTS)
        puts = (pltpu.make_async_copy(gi_buf.at[slot], gi_hbm.at[layer], gi_sem.at[slot]),
                pltpu.make_async_copy(go_buf.at[slot], go_hbm.at[layer], go_sem.at[slot]))

        @pl.when(i >= WIDEN_SLOTS)
        def _():
            for put in puts:
                put.wait()

        def fill(gi, go):
            for q in range(4):
                for s in range(SUB):
                    r = slice(s * rows, (s + 1) * rows)
                    gi_buf[slot, r, q * blk:(q + 1) * blk] = gi[i * SUB + s, q].astype(F32) * scale
                    go_buf[slot, q * blk + s * rows:q * blk + (s + 1) * rows, :] = go[i * SUB + s, q].astype(F32) * scale

        pl.when(core == 0)(lambda: fill(own, other))
        pl.when(core == 1)(lambda: fill(other, own))
        for put in puts:
            put.start()
        return carry

    lax.fori_loop(0, layers, step, 0)
    for slot in range(WIDEN_SLOTS):
        pltpu.make_async_copy(gi_buf.at[slot], gi_hbm.at[slot], gi_sem.at[slot]).wait()
        pltpu.make_async_copy(go_buf.at[slot], go_hbm.at[slot], go_sem.at[slot]).wait()
    put_dx.wait()


def solution(mesh):
    replicas = mesh.shape['dp']

    def device_fn(w_in, w_out, x_saved, h_saved, dy_in, acc_in, acc_out):
        layers, hidden, ff = w_in.shape[1:]
        tokens = dy_in.shape[1]
        blk = ff // 4
        chunks, rows = layers * SUB, blk // SUB
        room = chunks + len(LENT)
        dma = pltpu.SemaphoreType.DMA
        flops = 2 * tokens * hidden * ff * layers * 8
        call = pl.pallas_call(
            functools.partial(kernel, layers, blk),
            out_shape=(
                pltpu.VMEM((room, 4, rows, hidden), BF16),
                pltpu.VMEM((chunks, 4, rows, hidden), BF16),
                pltpu.VMEM((tokens, hidden), BF16),
                jax.ShapeDtypeStruct((layers, tokens, ff), BF16),
            ),
            in_specs=[pl.BlockSpec(memory_space=pl.ANY)] * 7,
            out_specs=[pl.BlockSpec(memory_space=pltpu.VMEM)] * 3 + [pl.BlockSpec(memory_space=pl.ANY)],
            scratch_shapes=[
                pltpu.VMEM((room, 4, rows, hidden), BF16),
                pltpu.VMEM((DEPTH, SUB, 4, rows, hidden), BF16),
                pltpu.VMEM((room, 2, rows, hidden), BF16),
                pltpu.VMEM((room, rows, hidden), BF16),
                pltpu.VMEM((2, SUB, 4, rows, hidden), BF16),
                pltpu.VMEM((2, hidden, ff), BF16),
                pltpu.VMEM((2, ff, hidden), BF16),
                pltpu.VMEM((4, tokens, ff), BF16),
                pltpu.VMEM((4, tokens, hidden), BF16),
                pltpu.VMEM((4, tokens, ff), BF16),
                pltpu.VMEM((2, hidden, ff), F32),
                pltpu.VMEM((2, ff, hidden), F32),
                pltpu.VMEM((layers, tokens, hidden), BF16),
                pltpu.VMEM((tokens, hidden), BF16),
                pltpu.VMEM((tokens, hidden), BF16),
                dma((2,)), dma((2,)), dma((4,)), dma((4,)), dma((2,)), dma((2,)), dma((2,)), dma((2,)), dma,
                dma((2,)), dma((DEPTH,)),
                dma((RING,)), dma((RING,)), dma((RING,)), dma((RING,)),
                dma((RING,)), dma((RING,)), dma((RING,)), dma((RING,)),
                dma, dma, dma, dma,
                dma((len(LENT),)), dma((len(LENT),)), dma((len(LENT),)), dma((len(LENT),)), pltpu.SemaphoreType.REGULAR,
            ],
            compiler_params=pltpu.CompilerParams(collective_id=0, has_side_effects=True, vmem_limit_bytes=67043328 - (36 << 19)),
            cost_estimate=pl.CostEstimate(flops=flops, bytes_accessed=200 << 20, transcendentals=0),
        )
        own, other, dx, _ = call(w_in, w_out, x_saved, h_saved, dy_in, acc_in, acc_out)
        grad_in, grad_out, dx_out = pl.pallas_call(
            functools.partial(widen, layers, blk, 1.0 / replicas),
            out_shape=(jax.ShapeDtypeStruct((layers, hidden, ff), F32), jax.ShapeDtypeStruct((layers, ff, hidden), F32),
                       jax.ShapeDtypeStruct((tokens, hidden), BF16)),
            in_specs=[pl.BlockSpec(memory_space=pltpu.VMEM)] * 3,
            out_specs=[pl.BlockSpec(memory_space=pl.ANY)] * 3,
            scratch_shapes=[pltpu.VMEM((WIDEN_SLOTS, hidden, ff), F32), pltpu.VMEM((WIDEN_SLOTS, ff, hidden), F32),
                            dma((WIDEN_SLOTS,)), dma((WIDEN_SLOTS,)), dma],
            compiler_params=pltpu.CompilerParams(vmem_limit_bytes=24 << 20),
        )(own, other, dx)
        return grad_in[None], grad_out[None], dx_out[None]

    return jax.shard_map(device_fn, mesh=mesh, in_specs=(P('pp'), P('pp'), P('pp', None, None, 'dp'), P('pp', None, None, 'dp'), P('pp', 'dp'), P('pp', 'dp'), P('pp', 'dp')), out_specs=(P('pp'), P('pp'), P('pp', 'dp')), check_vma=False)
```
